32 devices in a mesh: grp: 4 (over z), dev: 8 (over y, x, core).
Axes of the slice: x: 2, y: 2, z: 4, core: 2. Of those that a mesh axis runs over, the one named last changes fastest.
Arguments:
- blocks: bfloat16 [4096, 128, 128], P(('grp', 'dev')), may hold values from -0.29882812 to 0.29882812
- ids_one: int32 [2, 4096], P(None, ('grp', 'dev')), may hold values from 0 to 255, as said below
- ids_two: int32 [2, 2048], P(None, ('grp', 'dev')), may hold values from 0 to 127, as said below
- ids_three: int32 [2, 1024], P(None, ('grp', 'dev')), may hold values from 0 to 63
- match_one: int32 [256, 128], replicated, may hold values from 0 to 127, as said below
- match_two: int32 [128, 128], replicated, may hold values from 0 to 127, as said below
- match_three: int32 [64, 128], replicated, may hold values from 0 to 127, as said below
- target_one: int32 [4096], P(('grp', 'dev')), may hold values from 0 to 63
- target_two: int32 [2048], P(('grp', 'dev')), may hold values from 0 to 31
- target_three: int32 [1024], P(('grp', 'dev')), may hold values from 0 to 15
- vertex_weights: float32 [256, 128], P(('grp', 'dev')), may hold values from 0.1 to 120, as said below
Outputs:
- coarse_graph: float32 [512, 128, 128], P(('grp', 'dev'))
- rel_weight: float32 [32, 128], P(('grp', 'dev'))
The draws below stay inside these ranges and needn't reach their ends.
Inputs may be any that keep to these rules, and one draw needn't show every extreme that they name: `match_one`: rows 2b and 2b + 1 together name every number 0 to 127 exactly twice. `match_two`: rows 2b and 2b + 1 together name every number 0 to 127 exactly twice. `match_three`: rows 2b and 2b + 1 together name every number 0 to 127 exactly twice. `ids_one`: a fine block's row and column vertex blocks, halved by integer division, are the ids_two of the coarse slot it goes to. `ids_two`: a first-level block's row and column vertex blocks, halved by integer division, are the ids_three of the coarse slot it goes to. `vertex_weights`: positive.
All inputs are finite; a program needn't handle non-finite values.
Results may differ from the reference program's by a relative error of at most 0.0003.
Values may be sent and summed in bfloat16 or wider, within the bound.
A program may use at most 128 MiB of HBM per device.

```python
import math
import jax
import jax.numpy as jnp
from jax import lax

BLOCK = 128
SLOTS = 128
VWB = 8
NFINE = 4096
N_GRP = 4
N_DEV = 8
DEVICES = 32


def pairing(key, count):
    keys = jax.random.split(key, count // 2)
    perms = jax.vmap(lambda single: jax.random.permutation(single, 2 * BLOCK))(keys)
    return (perms // 2).reshape(count, BLOCK).astype(jnp.int32)


def route(count, per_dev, targets):
    slot = jnp.arange(count, dtype=jnp.int32)
    device = slot // per_dev
    local = slot % per_dev
    owner = device // N_DEV * N_DEV + local // (per_dev // N_DEV)
    return (owner * (per_dev // 2) + targets).astype(jnp.int32)


def layout(key):
    keys = jax.random.split(jax.random.fold_in(key, 7), 6)
    nfine = SLOTS * DEVICES
    vbzero = VWB * DEVICES
    ids_three = jax.random.randint(keys[0], (2, nfine // 4), 0, vbzero // 4, dtype=jnp.int32)
    target_two = jax.random.randint(keys[1], (nfine // 2,), 0, SLOTS // 4, dtype=jnp.int32)
    dest_two = route(nfine // 2, SLOTS // 2, target_two)
    ids_two = 2 * ids_three[:, dest_two] + jax.random.randint(keys[2], (2, nfine // 2), 0, 2, dtype=jnp.int32)
    target_one = jax.random.randint(keys[3], (nfine,), 0, SLOTS // 2, dtype=jnp.int32)
    dest_one = route(nfine, SLOTS, target_one)
    ids_one = 2 * ids_two[:, dest_one] + jax.random.randint(keys[4], (2, nfine), 0, 2, dtype=jnp.int32)
    target_three = jax.random.randint(keys[5], (nfine // 4,), 0, SLOTS // 8, dtype=jnp.int32)
    return (ids_one.astype(jnp.int32), ids_two.astype(jnp.int32), ids_three.astype(jnp.int32), target_one, target_two, target_three)


def draw_ids_one(key, part):
    return layout(key)[0]


def draw_ids_two(key, part):
    return layout(key)[1]


def draw_ids_three(key, part):
    return layout(key)[2]


def draw_target_one(key, part):
    return layout(key)[3]


def draw_target_two(key, part):
    return layout(key)[4]


def draw_target_three(key, part):
    return layout(key)[5]


def draw_match_one(key, part):
    return pairing(jax.random.fold_in(key, 11), VWB * DEVICES)


def draw_match_two(key, part):
    return pairing(jax.random.fold_in(key, 12), VWB * DEVICES // 2)


def draw_match_three(key, part):
    return pairing(jax.random.fold_in(key, 13), VWB * DEVICES // 4)


def draw_vertex_weights(key, part):
    first, second = jax.random.split(jax.random.fold_in(key, 21))
    count = VWB * DEVICES
    scale = jnp.exp(jax.random.uniform(first, (count, 1), jnp.float32, 0.0, math.log(16.0)))
    values = jax.random.uniform(second, (count, BLOCK), jnp.float32, 0.5, 1.5)
    return (scale * values).astype(jnp.float32)


def block_levels(own_key, extent, cuts, least, high):
    level = 1.0
    for position, shards_of in cuts:
        draws = jax.random.uniform(jax.random.fold_in(jax.random.fold_in(own_key, 6), position), (shards_of,), jnp.float32, least / len(cuts), high / len(cuts))
        level = level * jnp.repeat(jnp.exp(draws), extent[position] // shards_of).reshape((-1,) + (1,) * (len(extent) - 1 - position))
    return level


def scatter_about(own_key, dims, spread, reach, shards=(), kind=jnp.bfloat16):
    array = jax.random.normal(own_key, dims, jnp.float32) * spread
    if len(shards) > 0:
        array = block_levels(own_key, dims, shards, -0.22, 0.18) * array
    return jnp.clip(array, min=-reach, max=reach).astype(kind)


def setup_inputs(seed: int = 0) -> dict:
    key_list = jax.random.split(jax.random.key(seed), 12)
    return {
        "blocks": scatter_about(key_list[0], (NFINE, BLOCK, BLOCK), 0.05, 0.29882812, ((0, 32),)),
        "ids_one": draw_ids_one(jax.random.fold_in(key_list[11], 71), 0),
        "ids_two": draw_ids_two(jax.random.fold_in(key_list[11], 71), 0),
        "ids_three": draw_ids_three(jax.random.fold_in(key_list[11], 71), 0),
        "match_one": draw_match_one(jax.random.fold_in(key_list[11], 71), 0),
        "match_two": draw_match_two(jax.random.fold_in(key_list[11], 71), 0),
        "match_three": draw_match_three(jax.random.fold_in(key_list[11], 71), 0),
        "target_one": draw_target_one(jax.random.fold_in(key_list[11], 71), 0),
        "target_two": draw_target_two(jax.random.fold_in(key_list[11], 71), 0),
        "target_three": draw_target_three(jax.random.fold_in(key_list[11], 71), 0),
        "vertex_weights": draw_vertex_weights(jax.random.fold_in(key_list[11], 71), 0),
    }


def project_blocks(blocks, pair_ids, table):
    row_map = table[pair_ids[0]]
    col_map = table[pair_ids[1]]

    def single(matrix, rows, cols):
        halfway = jax.ops.segment_sum(matrix.astype(jnp.float32), rows, num_segments=BLOCK)
        return jax.ops.segment_sum(halfway.T, cols, num_segments=BLOCK).T

    return jax.vmap(single)(blocks, row_map, col_map)


def coarsen(blocks, pair_ids, table, targets, per_dev, fold_groups):
    count = blocks.shape[0]
    slot = jnp.arange(count, dtype=jnp.int32)
    device = slot // per_dev
    local = slot % per_dev
    group = device // N_DEV
    member = device % N_DEV
    if fold_groups:
        owner = (local // (per_dev // N_GRP)) * N_DEV + member
    else:
        owner = group * N_DEV + local // (per_dev // N_DEV)
    dest = (owner * (per_dev // 2) + targets).astype(jnp.int32)
    width = math.gcd(count, 512)
    turns = count // width
    inputs = (blocks.reshape(turns, width, BLOCK, BLOCK),
              pair_ids.reshape(2, turns, width).transpose(1, 0, 2),
              dest.reshape(turns, width))

    def accumulate(total, piece):
        part = project_blocks(piece[0], piece[1], table)
        return total.at[piece[2]].add(part), None

    start = jnp.zeros((count // 2, BLOCK, BLOCK), jnp.float32)
    coarse, _ = lax.scan(accumulate, start, inputs)
    return coarse


def pair_weights(weights, table):
    count = weights.shape[0]
    index = (jnp.arange(count, dtype=jnp.int32)[:, None] // 2) * BLOCK + table.astype(jnp.int32)
    summed = jax.ops.segment_sum(weights.reshape(-1), index.reshape(-1), num_segments=count // 2 * BLOCK)
    return summed.reshape(count // 2, BLOCK)


def reference(blocks, ids_one, ids_two, ids_three, match_one, match_two, match_three, target_one, target_two, target_three, vertex_weights):
    coarse_one = coarsen(blocks, ids_one, match_one, target_one, SLOTS, False)
    coarse_two = coarsen(coarse_one, ids_two, match_two, target_two, SLOTS // 2, False)
    coarse_graph = coarsen(coarse_two, ids_three, match_three, target_three, SLOTS // 4, True)
    weights_three = pair_weights(pair_weights(pair_weights(vertex_weights, match_one), match_two), match_three)
    total = jnp.sum(vertex_weights)
    rel_weight = weights_three * (weights_three.shape[0] * BLOCK) / total
    return coarse_graph, rel_weight
```

```python
import functools
import math

import jax
import jax.numpy as jnp
from jax import lax
from jax.experimental import pallas as pl
from jax.experimental.pallas import tpu as pltpu
from jax.sharding import PartitionSpec as P

LEVELS = 32767.0
TINY = 1e-30
NT = (((1,), (1,)), ((), ()))
ROWS = 8


def hot(row, rows, base):
    names = lax.broadcasted_iota(jnp.int32, (rows, row.shape[1]), 0) + base
    return (names == row).astype(jnp.bfloat16)


def halves(x):
    high = x.astype(jnp.bfloat16)
    low = (x - high.astype(jnp.float32)).astype(jnp.bfloat16)
    return high, low


def project(block, row, col, rows, base):
    left = hot(row, rows, base)
    halfway = jnp.dot(left, block, preferred_element_type=jnp.float32)
    right = hot(col, col.shape[1], 0)
    both = jnp.concatenate([right, right], axis=1)
    split = jnp.concatenate(halves(halfway), axis=1)
    return lax.dot_general(split, both, NT, preferred_element_type=jnp.float32)


def encode(part):
    peak = jnp.maximum(jnp.max(jnp.abs(part), axis=0, keepdims=True), TINY)
    code = jnp.round(part * (LEVELS / peak)).astype(jnp.int32)
    return code.astype(jnp.int16), peak * (1.0 / LEVELS)


def decode(code, scale):
    return code.astype(jnp.int32).astype(jnp.float32) * scale


def lookup(table, index):
    return jnp.take_along_axis(table, index, axis=1, mode="promise_in_bounds")


def fold(weights, row):
    width = row.shape[1]
    place = lax.broadcasted_iota(jnp.int32, (ROWS, width), 0)
    rest = jnp.broadcast_to(weights, (ROWS, width))
    split = jnp.zeros((ROWS, width), jnp.float32)
    for turn in range(3):
        part = rest.astype(jnp.bfloat16).astype(jnp.float32)
        rest = rest - part
        split = jnp.where(place == turn, part, split)
    right = hot(row, width, 0)
    return lax.dot_general(split.astype(jnp.bfloat16), right, NT, preferred_element_type=jnp.float32)


def column(row):
    lanes = row.shape[1]
    return jnp.broadcast_to(row, (lanes, lanes)).T


def latest(match, order):
    return jnp.max(jnp.where(match, order, -1), axis=0, keepdims=True)


def coarsen(
    n,
    groups,
    across,
    ids_smem,
    blocks,
    ids,
    target_one,
    target_two,
    target_three,
    weight,
    match_one,
    match_two,
    match_three,
    coarse,
    relative,
    table,
    own,
    theirs,
    labels,
    land_labels,
    land_far,
    land_weight,
    near_weight,
    land_weight_far,
    plan,
    plan_smem,
    theirs_smem,
    coarse_weight,
    sums,
    out_one,
    out_scale_one,
    land_one,
    land_scale_one,
    out_two,
    out_scale_two,
    land_two,
    land_scale_two,
    out_three,
    out_scale_three,
    land_three,
    land_scale_three,
    sums_three,
    near_send,
    near_recv,
    far_send,
    far_recv,
    raw_send,
    raw_recv,
    one_send,
    one_recv,
    two_send,
    two_recv,
    three_send,
    three_recv,
    own_sem,
    local,
):
    me = lax.axis_index("dev")
    group = lax.axis_index("grp")
    core, chip = me % 2, me // 2
    sibling = me + 1 - 2 * core
    chips = n // 2
    down = chips // across
    my_x, my_y = chip % across, chip // across
    count = own.shape[0]
    width = own.shape[2]
    rows = width // 2
    lanes = labels.shape[1]
    per_one, per_two, slots_two = count // n, count // 2 // n, count // 4
    per_three = slots_two // groups
    chunks = raw_send.shape[0]
    piece = count // chunks
    quarter = match_three.shape[0]
    sizes = ((across, down), (down, across))

    def peer(step):
        return lax.rem(me + step, n)

    def source(step):
        return lax.rem(me - step + n, n)

    def far_peer(step):
        return lax.rem(group + step, groups)

    def far_source(step):
        return lax.rem(group - step + groups, groups)

    def remote(src, dst, send, recv, device):
        return pltpu.make_async_remote_copy(
            src_ref=src,
            dst_ref=dst,
            send_sem=send,
            recv_sem=recv,
            device_id=device,
            device_id_type=pl.DeviceIdType.MESH,
        )

    def send_labels(v, here):
        return remote(labels, land_labels.at[here], near_send.at[0, v], near_recv.at[0, here], {"dev": v})

    def send_weight(v, here):
        return remote(weight, land_weight.at[here], near_send.at[1, v], near_recv.at[1, here], {"dev": v})

    def send_labels_far(v, here):
        return remote(labels, land_far.at[here], far_send.at[0, v], far_recv.at[0, here], {"grp": v})

    def send_weight_far(v, here):
        return remote(
            near_weight, land_weight_far.at[here], far_send.at[1, v], far_recv.at[1, here], {"grp": v}
        )

    def own_copy(c):
        return pltpu.make_async_copy(
            blocks.at[pl.ds(c * piece, piece)], own.at[pl.ds(c * piece, piece)], own_sem.at[c]
        )

    def send_raw(c):
        return remote(
            own.at[pl.ds(c * piece, piece)],
            theirs.at[pl.ds(c * piece, piece)],
            raw_send.at[c],
            raw_recv.at[c],
            {"dev": sibling},
        )

    def chip_at(b, first, second):
        return second * across + first if b == 0 else first * across + second

    def here_of(b):
        return (my_x, my_y) if b == 0 else (my_y, my_x)

    def send_one(i, b, step, turn):
        z, w = sizes[b]
        first, second = here_of(b)
        m = (step - 1) * w + turn
        to = chip_at(b, (first + step) % z, second) * 2 + core
        return (
            remote(
                out_one.at[i, b, m], land_one.at[i, b, m], one_send.at[i, b, m, 0],
                one_recv.at[i, b, m, 0], {"dev": to},
            ),
            remote(
                out_scale_one.at[i, b, m], land_scale_one.at[i, b, m], one_send.at[i, b, m, 1],
                one_recv.at[i, b, m, 1], {"dev": to},
            ),
        )

    def send_two(i, b, turn):
        w = sizes[b][1]
        first, second = here_of(b)
        m = turn - 1
        to = chip_at(b, first, (second + turn) % w) * 2 + core
        return (
            remote(
                out_two.at[i, b, m], land_two.at[i, b, m], two_send.at[i, b, m, 0],
                two_recv.at[i, b, m, 0], {"dev": to},
            ),
            remote(
                out_scale_two.at[i, b, m], land_scale_two.at[i, b, m], two_send.at[i, b, m, 1],
                two_recv.at[i, b, m, 1], {"dev": to},
            ),
        )

    def send_three(i, b, to_group, from_group, from_core):
        device = {"grp": to_group, "dev": chip * 2 + b}
        return (
            remote(
                out_three.at[i, b], land_three.at[from_group, from_core], three_send.at[i, b, 0],
                three_recv.at[from_group, from_core, 0], device,
            ),
            remote(
                out_scale_three.at[i, b], land_scale_three.at[from_group, from_core],
                three_send.at[i, b, 1], three_recv.at[from_group, from_core, 1], device,
            ),
        )

    def chunk_group(i):
        falling = groups - 1 - i
        low = jnp.where(falling > group, falling, falling - 1)
        high = jnp.where(i < group, i, i + 1)
        other = jnp.where(group < groups // 2, low, high)
        return jnp.where(i == groups - 1, group, other)

    for c in range(chunks):
        own_copy(c).start()

    barrier = pltpu.get_barrier_semaphore()

    @pl.loop(1, n)
    def _(step):
        pl.semaphore_signal(
            barrier, inc=1, device_id={"dev": peer(step)}, device_id_type=pl.DeviceIdType.MESH
        )

    @pl.loop(1, groups)
    def _(step):
        v = far_peer(step)
        pl.semaphore_signal(
            barrier, inc=1, device_id={"grp": v}, device_id_type=pl.DeviceIdType.MESH
        )
        pl.semaphore_signal(
            barrier, inc=1, device_id={"grp": v, "dev": sibling}, device_id_type=pl.DeviceIdType.MESH
        )

    labels[...] = jnp.zeros(labels.shape, jnp.int32)
    labels[0:2, 0:count] = ids[...]
    labels[2:3, 0:count] = target_one[...]
    labels[3:4, 0 : count // 2] = target_two[...]
    labels[4:5, 0 : count // 4] = target_three[...]
    land_labels[me] = labels[...]
    land_far[group] = labels[...]

    pl.semaphore_wait(barrier, n - 1 + 2 * (groups - 1))

    @pl.loop(1, n)
    def _(step):
        send_labels(peer(step), me).start()
        send_weight(peer(step), me).start()

    @pl.loop(1, groups)
    def _(step):
        send_labels_far(far_peer(step), group).start()

    for c in range(chunks):
        own_copy(c).wait()
        send_raw(c).start()

    for turn in range(4):
        one = match_one[pl.ds(turn, quarter, stride=4), :]
        two = match_two[pl.ds(turn // 2, quarter, stride=2), :]
        table[turn * quarter : (turn + 1) * quarter, :] = lookup(match_three[...], lookup(two, one))

    def mapping(b):
        return table[pl.ds((b % 4) * quarter + b // 4, 1), :]

    base = core * rows
    sums[2 * count] = jnp.zeros((rows, width), jnp.float32)
    sums_three[groups * per_three] = jnp.zeros(sums_three.shape[1:], jnp.float32)
    unroll = math.gcd(piece, 4)

    @pl.loop(0, count // unroll)
    def _(i):
        for j in range(unroll):
            k = i * unroll + j
            row, col = mapping(ids_smem[0, k]), mapping(ids_smem[1, k])
            sums[k] = project(own[k], row, col, rows, base)

    @pl.loop(1, n)
    def _(step):
        send_labels(source(step), source(step)).wait_recv()
        send_weight(source(step), source(step)).wait_recv()

    @pl.loop(1, groups)
    def _(step):
        send_labels_far(far_source(step), far_source(step)).wait_recv()

    ids_down = pltpu.make_async_copy(land_labels.at[sibling], theirs_smem, local.at[0])
    ids_down.start()

    square = (lanes, lanes)
    lane = lax.broadcasted_iota(jnp.int32, (1, lanes), 1)
    order_down = lax.broadcasted_iota(jnp.int32, square, 0)
    order_across = lax.broadcasted_iota(jnp.int32, square, 1)

    def slots_of(mine):
        first = mine[2:3, :]
        spread = jnp.broadcast_to(first, mine.shape)
        second = jnp.zeros((1, lanes), jnp.int32)
        for o in range(n):
            second = jnp.where(lane // per_one == o, lookup(land_labels[o], spread)[3:4, :], second)
        return first // per_two * slots_two + second

    slot_own, slot_theirs = slots_of(labels[...]), slots_of(land_labels[sibling])
    down_own, down_theirs = column(slot_own), column(slot_theirs)
    none = 2 * count
    before = latest((down_own == slot_own) & (order_down < order_across), order_down)
    plan[0:1, :] = jnp.where(before < 0, none, before)
    before = jnp.maximum(
        latest((down_theirs == slot_theirs) & (order_down < order_across), order_down + count),
        latest(down_own == slot_theirs, order_down),
    )
    plan[1:2, :] = jnp.where(before < 0, none, before)
    blocks_of_slots = -(-n * slots_two // lanes)
    for part in range(blocks_of_slots):
        name = order_across + part * lanes
        last = jnp.maximum(
            latest(down_own == name, order_down), latest(down_theirs == name, order_down + count)
        )
        plan[2 + part : 3 + part, :] = jnp.where(last < 0, none, last)
    total = groups * per_three
    pick = jnp.broadcast_to(group * per_three + lane % per_three, (ROWS, lanes))
    third = jnp.full((1, lanes), -1, jnp.int32)
    for u in range(groups):
        third = jnp.where(lane // per_three == u, lookup(land_far[u], pick)[4:5, :], third)
    down_third = column(third)

    def rank(k):
        return (group - k // per_three - 1 + groups) % groups * per_three + k % per_three

    rank_down, rank_across = rank(order_down), rank(order_across)
    real = order_down < total
    before = latest(real & (down_third == third) & (rank_down < rank_across), rank_down)
    last = latest(real & (down_third == order_across), rank_down)
    third_row = 2 + blocks_of_slots
    plan[third_row : third_row + 1, :] = jnp.where(before < 0, total, before)
    plan[third_row + 1 : third_row + 2, :] = jnp.where(last < 0, total, last)
    rest = plan.shape[0] - third_row - 2
    if rest:
        plan[third_row + 2 :, :] = jnp.zeros((rest, lanes), jnp.int32)
    to_smem = pltpu.make_async_copy(plan, plan_smem, local.at[1])
    to_smem.start()

    held = weight[...]
    for step in range(1, n):
        held = held + land_weight[peer(step)]
    near_weight[...] = held

    @pl.loop(1, groups)
    def _(step):
        send_weight_far(far_peer(step), group).start()

    ids_down.wait()
    to_smem.wait()

    @pl.loop(0, count)
    def _(k):
        sums[k] = sums[k] + sums[plan_smem[0, k]]

    @pl.loop(0, chunks)
    def _(c):
        send_raw(c).wait_recv()

        @pl.loop(0, piece // unroll)
        def _(i):
            parts = []
            for j in range(unroll):
                k = c * piece + i * unroll + j
                row, col = mapping(theirs_smem[0, k]), mapping(theirs_smem[1, k])
                parts.append(project(theirs[k], row, col, rows, base))
            for j in range(unroll):
                k = c * piece + i * unroll + j
                sums[count + k] = parts[j] + sums[plan_smem[1, k]]

    def held_here(to_chip, b, i, j):
        slot = (to_chip * 2 + b) * slots_two + chunk_group(i) * per_three + j
        return sums[plan_smem[2 + slot // lanes, slot % lanes]]

    def pack(parts, codes, scales):
        for j, part in enumerate(parts):
            code, scale = encode(part)
            codes[j] = code
            scales[j : j + 1, :] = scale

    def start(copies):
        for copy in copies:
            copy.start()

    def arrive(copies):
        for copy in copies:
            copy.wait_recv()

    def turns(b):
        w = sizes[b][1]
        return [*range(1, w), 0]

    def first_hop(i):
        for spot in range(max(across, down)):
            for b in range(2):
                z, w = sizes[b]
                if spot >= w:
                    continue
                turn = turns(b)[spot]
                first, second = here_of(b)
                for step in range(1, z):
                    to = chip_at(b, (first + step) % z, (second + turn) % w)
                    m = (step - 1) * w + turn
                    parts = [held_here(to, b, i, j) for j in range(per_three)]
                    pack(parts, out_one.at[i, b, m], out_scale_one.at[i, b, m])
                    start(send_one(i, b, step, turn))

    def with_first(parts, i, b, turn):
        z, w = sizes[b]
        for step in range(1, z):
            m = (step - 1) * w + turn
            arrive(send_one(i, b, step, turn))
            parts = [
                p + decode(land_one[i, b, m, j], land_scale_one[i, b, m, j : j + 1, :])
                for j, p in enumerate(parts)
            ]
        return parts

    def second_hop(i):
        for b in range(2):
            w = sizes[b][1]
            first, second = here_of(b)
            for turn in range(1, w):
                to = chip_at(b, first, (second + turn) % w)
                parts = [held_here(to, b, i, j) for j in range(per_three)]
                parts = with_first(parts, i, b, turn)
                pack(parts, out_two.at[i, b, turn - 1], out_scale_two.at[i, b, turn - 1])
                start(send_two(i, b, turn))

    def reduced(i):
        for b in range(2):
            w = sizes[b][1]
            parts = [held_here(chip, b, i, j) for j in range(per_three)]
            parts = with_first(parts, i, b, 0)
            for turn in range(1, w):
                arrive(send_two(i, b, turn))
                parts = [
                    p + decode(land_two[i, b, turn - 1, j], land_scale_two[i, b, turn - 1, j : j + 1, :])
                    for j, p in enumerate(parts)
                ]
            pack(parts, out_three.at[i, b], out_scale_three.at[i, b])

    def third_hop(i):
        reduced(i)
        for b in range(2):
            start(send_three(i, b, chunk_group(i), group, core))

    @pl.loop(0, groups)
    def _(i):
        first_hop(i)

        @pl.when(i > 0)
        def _():
            third_hop(i - 1)

        second_hop(i)

    owned = weight.shape[0]
    start_row = (group * n + me) * (owned // 4)
    for e in range(owned // 8):
        folded = jnp.zeros((ROWS, width), jnp.float32)
        for f in range(8 * e, 8 * e + 8):
            row = table[pl.ds(f % 4 * quarter + start_row + f // 4, 1), :]
            folded = folded + fold(weight[f : f + 1, :], row)
        coarse_weight[e : e + 1, :] = jnp.sum(folded, axis=0, keepdims=True)
    held = near_weight[...]
    for step in range(1, groups):
        send_weight_far(far_source(step), far_source(step)).wait_recv()
        held = held + land_weight_far[far_source(step)]
    whole = jnp.sum(jnp.sum(held, axis=0, keepdims=True), axis=1, keepdims=True)
    vertices = relative.shape[0] * n * groups * relative.shape[1]
    relative[...] = coarse_weight[...] * vertices / whole

    end = groups - 1
    reduced(end)
    start(send_three(end, 1 - core, group, group, core))

    def take(codes, scales, at, h, u):
        for j in range(per_three):
            part = decode(codes[j], scales[j : j + 1, :])
            sums_three[at + j, h] = part + sums_three[plan_smem[third_row, u * per_three + j], h]

    @pl.loop(1, groups)
    def _(step):
        u = far_source(step)
        for h in range(2):
            arrive(send_three(0, h, u, u, h))
            take(land_three.at[u, h], land_scale_three.at[u, h], (step - 1) * per_three, h, u)

    take(out_three.at[end, core], out_scale_three.at[end, core], end * per_three, core, group)
    other = 1 - core
    arrive(send_three(end, other, group, group, other))
    take(land_three.at[group, other], land_scale_three.at[group, other], end * per_three, other, group)

    @pl.loop(0, coarse.shape[0])
    def _(slot):
        coarse[slot] = sums_three[plan_smem[third_row + 1, slot]]

    @pl.loop(1, n)
    def _(step):
        send_labels(peer(step), me).wait_send()
        send_weight(peer(step), me).wait_send()

    @pl.loop(1, groups)
    def _(step):
        send_labels_far(far_peer(step), group).wait_send()
        send_weight_far(far_peer(step), group).wait_send()

    @pl.loop(0, chunks)
    def _(c):
        send_raw(c).wait_send()

    def sent(copies):
        for copy in copies:
            copy.wait_send()

    @pl.loop(0, groups)
    def _(i):
        for b in range(2):
            z, w = sizes[b]
            for step in range(1, z):
                for turn in range(w):
                    sent(send_one(i, b, step, turn))
            for turn in range(1, w):
                sent(send_two(i, b, turn))

    @pl.loop(0, groups - 1)
    def _(i):
        for b in range(2):
            sent(send_three(i, b, group, group, core))

    sent(send_three(end, 1 - core, group, group, core))


SMEM = pl.BlockSpec(memory_space=pltpu.SMEM)
VMEM = pl.BlockSpec(memory_space=pltpu.VMEM)
HBM = pl.BlockSpec(memory_space=pl.ANY)


def per_device(
    blocks,
    ids_one,
    ids_two,
    ids_three,
    match_one,
    match_two,
    match_three,
    target_one,
    target_two,
    target_three,
    vertex_weights,
):
    n, groups = lax.axis_size("dev"), lax.axis_size("grp")
    count, width = blocks.shape[0], blocks.shape[1]
    rows = width // 2
    lanes = -(-count // width) * width
    owned = vertex_weights.shape[0]
    slots = count // 4
    per = slots // groups
    chips = n // 2
    across = 1
    while across * across < chips:
        across *= 2
    down = chips // across
    hop_one = max((across - 1) * down, (down - 1) * across, 1)
    hop_two = max(across - 1, down - 1, 1)
    plan_rows = -(-(4 + -(-n * slots // lanes)) // ROWS) * ROWS
    chunks = math.gcd(count, 8)
    code = (per, rows, width)

    def message(*lead):
        return [pltpu.VMEM(lead + code, jnp.int16), pltpu.VMEM(lead + (per, width), jnp.float32)] * 2

    coarse, relative = pl.pallas_call(
        functools.partial(coarsen, n, groups, across),
        in_specs=[SMEM, HBM] + [VMEM] * 8,
        out_specs=(VMEM, VMEM),
        out_shape=(
            jax.ShapeDtypeStruct((count // 8, 2, rows, width), jnp.float32),
            jax.ShapeDtypeStruct((owned // 8, width), jnp.float32),
        ),
        scratch_shapes=[
            pltpu.VMEM(match_one.shape, jnp.int32),
            pltpu.VMEM((count, width, width), jnp.bfloat16),
            pltpu.VMEM((count, width, width), jnp.bfloat16),
            pltpu.VMEM((ROWS, lanes), jnp.int32),
            pltpu.VMEM((n, ROWS, lanes), jnp.int32),
            pltpu.VMEM((groups, ROWS, lanes), jnp.int32),
            pltpu.VMEM((n, owned, width), jnp.float32),
            pltpu.VMEM((owned, width), jnp.float32),
            pltpu.VMEM((groups, owned, width), jnp.float32),
            pltpu.VMEM((plan_rows, lanes), jnp.int32),
            pltpu.SMEM((plan_rows, lanes), jnp.int32),
            pltpu.SMEM((ROWS, lanes), jnp.int32),
            pltpu.VMEM((owned // 8, width), jnp.float32),
            pltpu.VMEM((2 * count + 1, rows, width), jnp.float32),
            *message(groups, 2, hop_one),
            *message(groups, 2, hop_two),
            *message(groups, 2),
            pltpu.VMEM((groups * per + 1, 2, rows, width), jnp.float32),
            pltpu.SemaphoreType.DMA((2, n)),
            pltpu.SemaphoreType.DMA((2, n)),
            pltpu.SemaphoreType.DMA((2, groups)),
            pltpu.SemaphoreType.DMA((2, groups)),
            pltpu.SemaphoreType.DMA((chunks,)),
            pltpu.SemaphoreType.DMA((chunks,)),
            pltpu.SemaphoreType.DMA((groups, 2, hop_one, 2)),
            pltpu.SemaphoreType.DMA((groups, 2, hop_one, 2)),
            pltpu.SemaphoreType.DMA((groups, 2, hop_two, 2)),
            pltpu.SemaphoreType.DMA((groups, 2, hop_two, 2)),
            pltpu.SemaphoreType.DMA((groups, 2, 2)),
            pltpu.SemaphoreType.DMA((groups, 2, 2)),
            pltpu.SemaphoreType.DMA((chunks,)),
            pltpu.SemaphoreType.DMA((2,)),
        ],
        compiler_params=pltpu.CompilerParams(
            collective_id=0, has_side_effects=True, vmem_limit_bytes=63 * 1024 * 1024
        ),
    )(
        ids_one,
        blocks,
        ids_one,
        target_one[None],
        target_two[None],
        target_three[None],
        vertex_weights,
        match_one,
        match_two,
        match_three,
    )
    return coarse.reshape(count // 8, width, width), relative


def solution(mesh):
    both = ("grp", "dev")
    return jax.shard_map(
        per_device,
        mesh=mesh,
        in_specs=(
            P(both, None, None),
            P(None, both),
            P(None, both),
            P(None, both),
            P(),
            P(),
            P(),
            P(both),
            P(both),
            P(both),
            P(both, None),
        ),
        out_specs=(P(both, None, None), P(both, None)),
        check_vma=False,
    )
```

```python
import functools
import math

import jax
import jax.numpy as jnp
from jax import lax
from jax.experimental import pallas as pl
from jax.experimental.pallas import tpu as pltpu
from jax.sharding import PartitionSpec as P

LEVELS = 32767.0
TINY = 1e-30
NT = (((1,), (1,)), ((), ()))
ROWS = 8


def hot(row, rows, base):
    names = lax.broadcasted_iota(jnp.int32, (rows, row.shape[1]), 0) + base
    return (names == row).astype(jnp.bfloat16)


def halves(x):
    high = x.astype(jnp.bfloat16)
    low = (x - high.astype(jnp.float32)).astype(jnp.bfloat16)
    return high, low


def project(block, row, col, rows, base):
    left = hot(row, rows, base)
    halfway = jnp.dot(left, block, preferred_element_type=jnp.float32)
    right = hot(col, col.shape[1], 0)
    both = jnp.concatenate([right, right], axis=1)
    split = jnp.concatenate(halves(halfway), axis=1)
    return lax.dot_general(split, both, NT, preferred_element_type=jnp.float32)


def encode(part):
    peak = jnp.maximum(jnp.max(jnp.abs(part), axis=0, keepdims=True), TINY)
    code = jnp.round(part * (LEVELS / peak)).astype(jnp.int32)
    return code.astype(jnp.int16), peak * (1.0 / LEVELS)


def decode(code, scale):
    return code.astype(jnp.int32).astype(jnp.float32) * scale


def lookup(table, index):
    return jnp.take_along_axis(table, index, axis=1, mode="promise_in_bounds")


def fold(weights, row):
    width = row.shape[1]
    place = lax.broadcasted_iota(jnp.int32, (ROWS, width), 0)
    rest = jnp.broadcast_to(weights, (ROWS, width))
    split = jnp.zeros((ROWS, width), jnp.float32)
    for turn in range(3):
        part = rest.astype(jnp.bfloat16).astype(jnp.float32)
        rest = rest - part
        split = jnp.where(place == turn, part, split)
    right = hot(row, width, 0)
    return lax.dot_general(split.astype(jnp.bfloat16), right, NT, preferred_element_type=jnp.float32)


def column(row):
    lanes = row.shape[1]
    return jnp.broadcast_to(row, (lanes, lanes)).T


def latest(match, order):
    return jnp.max(jnp.where(match, order, -1), axis=0, keepdims=True)


def coarsen(
    n,
    groups,
    across,
    ids_smem,
    blocks,
    ids,
    target_one,
    target_two,
    target_three,
    weight,
    match_one,
    match_two,
    match_three,
    coarse,
    relative,
    table,
    own,
    theirs,
    labels,
    land_labels,
    land_far,
    land_weight,
    near_weight,
    land_weight_far,
    plan,
    plan_smem,
    theirs_smem,
    coarse_weight,
    sums,
    out_one,
    out_scale_one,
    land_one,
    land_scale_one,
    out_two,
    out_scale_two,
    land_two,
    land_scale_two,
    out_three,
    out_scale_three,
    land_three,
    land_scale_three,
    sums_three,
    near_send,
    near_recv,
    far_send,
    far_recv,
    raw_send,
    raw_recv,
    one_send,
    one_recv,
    two_send,
    two_recv,
    three_send,
    three_recv,
    own_sem,
    local,
):
    me = lax.axis_index("dev")
    group = lax.axis_index("grp")
    core, chip = me % 2, me // 2
    sibling = me + 1 - 2 * core
    chips = n // 2
    down = chips // across
    my_x, my_y = chip % across, chip // across
    count = own.shape[0]
    width = own.shape[2]
    rows = width // 2
    lanes = labels.shape[1]
    per_one, per_two, slots_two = count // n, count // 2 // n, count // 4
    per_three = slots_two // groups
    chunks = raw_send.shape[0]
    piece = count // chunks
    quarter = match_three.shape[0]
    sizes = ((across, down), (down, across))

    def peer(step):
        return lax.rem(me + step, n)

    def source(step):
        return lax.rem(me - step + n, n)

    def far_peer(step):
        return lax.rem(group + step, groups)

    def far_source(step):
        return lax.rem(group - step + groups, groups)

    def remote(src, dst, send, recv, device):
        return pltpu.make_async_remote_copy(
            src_ref=src,
            dst_ref=dst,
            send_sem=send,
            recv_sem=recv,
            device_id=device,
            device_id_type=pl.DeviceIdType.MESH,
        )

    def send_labels(v, here):
        return remote(labels, land_labels.at[here], near_send.at[0, v], near_recv.at[0, here], {"dev": v})

    def send_weight(v, here):
        return remote(weight, land_weight.at[here], near_send.at[1, v], near_recv.at[1, here], {"dev": v})

    def send_labels_far(v, here):
        return remote(labels, land_far.at[here], far_send.at[0, v], far_recv.at[0, here], {"grp": v})

    def send_weight_far(v, here):
        return remote(
            near_weight, land_weight_far.at[here], far_send.at[1, v], far_recv.at[1, here], {"grp": v}
        )

    def own_copy(c):
        return pltpu.make_async_copy(
            blocks.at[pl.ds(c * piece, piece)], own.at[pl.ds(c * piece, piece)], own_sem.at[c]
        )

    def send_raw(c):
        return remote(
            own.at[pl.ds(c * piece, piece)],
            theirs.at[pl.ds(c * piece, piece)],
            raw_send.at[c],
            raw_recv.at[c],
            {"dev": sibling},
        )

    def chip_at(b, first, second):
        return second * across + first if b == 0 else first * across + second

    def here_of(b):
        return (my_x, my_y) if b == 0 else (my_y, my_x)

    def send_one(i, b, step, turn):
        z, w = sizes[b]
        first, second = here_of(b)
        m = (step - 1) * w + turn
        to = chip_at(b, (first + step) % z, second) * 2 + core
        return (
            remote(
                out_one.at[i, b, m], land_one.at[i, b, m], one_send.at[i, b, m, 0],
                one_recv.at[i, b, m, 0], {"dev": to},
            ),
            remote(
                out_scale_one.at[i, b, m], land_scale_one.at[i, b, m], one_send.at[i, b, m, 1],
                one_recv.at[i, b, m, 1], {"dev": to},
            ),
        )

    def send_two(i, b, turn):
        w = sizes[b][1]
        first, second = here_of(b)
        m = turn - 1
        to = chip_at(b, first, (second + turn) % w) * 2 + core
        return (
            remote(
                out_two.at[i, b, m], land_two.at[i, b, m], two_send.at[i, b, m, 0],
                two_recv.at[i, b, m, 0], {"dev": to},
            ),
            remote(
                out_scale_two.at[i, b, m], land_scale_two.at[i, b, m], two_send.at[i, b, m, 1],
                two_recv.at[i, b, m, 1], {"dev": to},
            ),
        )

    def send_three(i, b, to_group, from_group, from_core):
        device = {"grp": to_group, "dev": chip * 2 + b}
        return (
            remote(
                out_three.at[i, b], land_three.at[from_group, from_core], three_send.at[i, b, 0],
                three_recv.at[from_group, from_core, 0], device,
            ),
            remote(
                out_scale_three.at[i, b], land_scale_three.at[from_group, from_core],
                three_send.at[i, b, 1], three_recv.at[from_group, from_core, 1], device,
            ),
        )

    def chunk_group(i):
        falling = groups - 1 - i
        low = jnp.where(falling > group, falling, falling - 1)
        high = jnp.where(i < group, i, i + 1)
        other = jnp.where(group < groups // 2, low, high)
        return jnp.where(i == groups - 1, group, other)

    for c in range(chunks):
        own_copy(c).start()

    barrier = pltpu.get_barrier_semaphore()

    @pl.loop(1, n)
    def _(step):
        pl.semaphore_signal(
            barrier, inc=1, device_id={"dev": peer(step)}, device_id_type=pl.DeviceIdType.MESH
        )

    @pl.loop(1, groups)
    def _(step):
        v = far_peer(step)
        pl.semaphore_signal(
            barrier, inc=1, device_id={"grp": v}, device_id_type=pl.DeviceIdType.MESH
        )
        pl.semaphore_signal(
            barrier, inc=1, device_id={"grp": v, "dev": sibling}, device_id_type=pl.DeviceIdType.MESH
        )

    labels[...] = jnp.zeros(labels.shape, jnp.int32)
    labels[0:2, 0:count] = ids[...]
    labels[2:3, 0:count] = target_one[...]
    labels[3:4, 0 : count // 2] = target_two[...]
    labels[4:5, 0 : count // 4] = target_three[...]
    land_labels[me] = labels[...]
    land_far[group] = labels[...]

    pl.semaphore_wait(barrier, n - 1 + 2 * (groups - 1))

    @pl.loop(1, n)
    def _(step):
        send_labels(peer(step), me).start()
        send_weight(peer(step), me).start()

    @pl.loop(1, groups)
    def _(step):
        send_labels_far(far_peer(step), group).start()

    for c in range(chunks):
        own_copy(c).wait()
        send_raw(c).start()

    for turn in range(4):
        one = match_one[pl.ds(turn, quarter, stride=4), :]
        two = match_two[pl.ds(turn // 2, quarter, stride=2), :]
        table[turn * quarter : (turn + 1) * quarter, :] = lookup(match_three[...], lookup(two, one))

    def mapping(b):
        return table[pl.ds((b % 4) * quarter + b // 4, 1), :]

    base = core * rows
    sums[2 * count] = jnp.zeros((rows, width), jnp.float32)
    sums_three[groups * per_three] = jnp.zeros(sums_three.shape[1:], jnp.float32)
    unroll = math.gcd(piece, 16)

    @pl.loop(0, count // unroll)
    def _(i):
        parts = []
        for j in range(unroll):
            k = i * unroll + j
            row, col = mapping(ids_smem[0, k]), mapping(ids_smem[1, k])
            parts.append(project(own[k], row, col, rows, base))
        for j in range(unroll):
            sums[i * unroll + j] = parts[j]

    @pl.loop(1, n)
    def _(step):
        send_labels(source(step), source(step)).wait_recv()
        send_weight(source(step), source(step)).wait_recv()

    @pl.loop(1, groups)
    def _(step):
        send_labels_far(far_source(step), far_source(step)).wait_recv()

    ids_down = pltpu.make_async_copy(land_labels.at[sibling], theirs_smem, local.at[0])
    ids_down.start()

    square = (lanes, lanes)
    lane = lax.broadcasted_iota(jnp.int32, (1, lanes), 1)
    order_down = lax.broadcasted_iota(jnp.int32, square, 0)
    order_across = lax.broadcasted_iota(jnp.int32, square, 1)

    def slots_of(mine):
        first = mine[2:3, :]
        spread = jnp.broadcast_to(first, mine.shape)
        second = jnp.zeros((1, lanes), jnp.int32)
        for o in range(n):
            second = jnp.where(lane // per_one == o, lookup(land_labels[o], spread)[3:4, :], second)
        return first // per_two * slots_two + second

    slot_own, slot_theirs = slots_of(labels[...]), slots_of(land_labels[sibling])
    down_own, down_theirs = column(slot_own), column(slot_theirs)
    none = 2 * count
    before = latest((down_own == slot_own) & (order_down < order_across), order_down)
    plan[0:1, :] = jnp.where(before < 0, none, before)
    before = jnp.maximum(
        latest((down_theirs == slot_theirs) & (order_down < order_across), order_down + count),
        latest(down_own == slot_theirs, order_down),
    )
    plan[1:2, :] = jnp.where(before < 0, none, before)
    blocks_of_slots = -(-n * slots_two // lanes)
    for part in range(blocks_of_slots):
        name = order_across + part * lanes
        last = jnp.maximum(
            latest(down_own == name, order_down), latest(down_theirs == name, order_down + count)
        )
        plan[2 + part : 3 + part, :] = jnp.where(last < 0, none, last)
    total = groups * per_three
    pick = jnp.broadcast_to(group * per_three + lane % per_three, (ROWS, lanes))
    third = jnp.full((1, lanes), -1, jnp.int32)
    for u in range(groups):
        third = jnp.where(lane // per_three == u, lookup(land_far[u], pick)[4:5, :], third)
    down_third = column(third)

    def rank(k):
        return (group - k // per_three - 1 + groups) % groups * per_three + k % per_three

    rank_down, rank_across = rank(order_down), rank(order_across)
    real = order_down < total
    before = latest(real & (down_third == third) & (rank_down < rank_across), rank_down)
    last = latest(real & (down_third == order_across), rank_down)
    third_row = 2 + blocks_of_slots
    plan[third_row : third_row + 1, :] = jnp.where(before < 0, total, before)
    plan[third_row + 1 : third_row + 2, :] = jnp.where(last < 0, total, last)
    rest = plan.shape[0] - third_row - 2
    if rest:
        plan[third_row + 2 :, :] = jnp.zeros((rest, lanes), jnp.int32)
    to_smem = pltpu.make_async_copy(plan, plan_smem, local.at[1])
    to_smem.start()

    held = weight[...]
    for step in range(1, n):
        held = held + land_weight[peer(step)]
    near_weight[...] = held

    @pl.loop(1, groups)
    def _(step):
        send_weight_far(far_peer(step), group).start()

    ids_down.wait()
    to_smem.wait()

    @pl.loop(0, count // unroll)
    def _(i):
        for j in range(unroll):
            k = i * unroll + j
            sums[k] = sums[k] + sums[plan_smem[0, k]]

    @pl.loop(0, chunks)
    def _(c):
        send_raw(c).wait_recv()

        @pl.loop(0, piece // unroll)
        def _(i):
            parts = []
            for j in range(unroll):
                k = c * piece + i * unroll + j
                row, col = mapping(theirs_smem[0, k]), mapping(theirs_smem[1, k])
                parts.append(project(theirs[k], row, col, rows, base))
            for j in range(unroll):
                k = c * piece + i * unroll + j
                sums[count + k] = parts[j] + sums[plan_smem[1, k]]

    def held_here(to_chip, b, i, j):
        slot = (to_chip * 2 + b) * slots_two + chunk_group(i) * per_three + j
        return sums[plan_smem[2 + slot // lanes, slot % lanes]]

    def pack(parts, codes, scales):
        for j, part in enumerate(parts):
            code, scale = encode(part)
            codes[j] = code
            scales[j : j + 1, :] = scale

    def start(copies):
        for copy in copies:
            copy.start()

    def arrive(copies):
        for copy in copies:
            copy.wait_recv()

    def turns(b):
        w = sizes[b][1]
        return [*range(1, w), 0]

    def first_hop(i):
        for spot in range(max(across, down)):
            for b in range(2):
                z, w = sizes[b]
                if spot >= w:
                    continue
                turn = turns(b)[spot]
                first, second = here_of(b)
                for step in range(1, z):
                    to = chip_at(b, (first + step) % z, (second + turn) % w)
                    m = (step - 1) * w + turn
                    parts = [held_here(to, b, i, j) for j in range(per_three)]
                    pack(parts, out_one.at[i, b, m], out_scale_one.at[i, b, m])
                    start(send_one(i, b, step, turn))

    def with_first(parts, i, b, turn):
        z, w = sizes[b]
        for step in range(1, z):
            m = (step - 1) * w + turn
            arrive(send_one(i, b, step, turn))
            parts = [
                p + decode(land_one[i, b, m, j], land_scale_one[i, b, m, j : j + 1, :])
                for j, p in enumerate(parts)
            ]
        return parts

    def second_hop(i):
        for b in range(2):
            w = sizes[b][1]
            first, second = here_of(b)
            for turn in range(1, w):
                to = chip_at(b, first, (second + turn) % w)
                parts = [held_here(to, b, i, j) for j in range(per_three)]
                parts = with_first(parts, i, b, turn)
                pack(parts, out_two.at[i, b, turn - 1], out_scale_two.at[i, b, turn - 1])
                start(send_two(i, b, turn))

    def reduced(i):
        for b in range(2):
            w = sizes[b][1]
            parts = [held_here(chip, b, i, j) for j in range(per_three)]
            parts = with_first(parts, i, b, 0)
            for turn in range(1, w):
                arrive(send_two(i, b, turn))
                parts = [
                    p + decode(land_two[i, b, turn - 1, j], land_scale_two[i, b, turn - 1, j : j + 1, :])
                    for j, p in enumerate(parts)
                ]
            pack(parts, out_three.at[i, b], out_scale_three.at[i, b])

    def third_hop(i):
        reduced(i)
        for b in range(2):
            start(send_three(i, b, chunk_group(i), group, core))

    @pl.loop(0, groups)
    def _(i):
        first_hop(i)

        @pl.when(i > 0)
        def _():
            third_hop(i - 1)

        second_hop(i)

    owned = weight.shape[0]
    start_row = (group * n + me) * (owned // 4)
    for e in range(owned // 8):
        folded = jnp.zeros((ROWS, width), jnp.float32)
        for f in range(8 * e, 8 * e + 8):
            row = table[pl.ds(f % 4 * quarter + start_row + f // 4, 1), :]
            folded = folded + fold(weight[f : f + 1, :], row)
        coarse_weight[e : e + 1, :] = jnp.sum(folded, axis=0, keepdims=True)
    held = near_weight[...]
    for step in range(1, groups):
        send_weight_far(far_source(step), far_source(step)).wait_recv()
        held = held + land_weight_far[far_source(step)]
    whole = jnp.sum(jnp.sum(held, axis=0, keepdims=True), axis=1, keepdims=True)
    vertices = relative.shape[0] * n * groups * relative.shape[1]
    relative[...] = coarse_weight[...] * vertices / whole

    end = groups - 1
    reduced(end)
    start(send_three(end, 1 - core, group, group, core))

    def take(codes, scales, at, h, u):
        for j in range(per_three):
            part = decode(codes[j], scales[j : j + 1, :])
            sums_three[at + j, h] = part + sums_three[plan_smem[third_row, u * per_three + j], h]

    @pl.loop(1, groups)
    def _(step):
        u = far_source(step)
        for h in range(2):
            arrive(send_three(0, h, u, u, h))
            take(land_three.at[u, h], land_scale_three.at[u, h], (step - 1) * per_three, h, u)

    take(out_three.at[end, core], out_scale_three.at[end, core], end * per_three, core, group)
    other = 1 - core
    arrive(send_three(end, other, group, group, other))
    take(land_three.at[group, other], land_scale_three.at[group, other], end * per_three, other, group)

    @pl.loop(0, coarse.shape[0])
    def _(slot):
        coarse[slot] = sums_three[plan_smem[third_row + 1, slot]]

    @pl.loop(1, n)
    def _(step):
        send_labels(peer(step), me).wait_send()
        send_weight(peer(step), me).wait_send()

    @pl.loop(1, groups)
    def _(step):
        send_labels_far(far_peer(step), group).wait_send()
        send_weight_far(far_peer(step), group).wait_send()

    @pl.loop(0, chunks)
    def _(c):
        send_raw(c).wait_send()

    def sent(copies):
        for copy in copies:
            copy.wait_send()

    @pl.loop(0, groups)
    def _(i):
        for b in range(2):
            z, w = sizes[b]
            for step in range(1, z):
                for turn in range(w):
                    sent(send_one(i, b, step, turn))
            for turn in range(1, w):
                sent(send_two(i, b, turn))

    @pl.loop(0, groups - 1)
    def _(i):
        for b in range(2):
            sent(send_three(i, b, group, group, core))

    sent(send_three(end, 1 - core, group, group, core))


SMEM = pl.BlockSpec(memory_space=pltpu.SMEM)
VMEM = pl.BlockSpec(memory_space=pltpu.VMEM)
HBM = pl.BlockSpec(memory_space=pl.ANY)


def per_device(
    blocks,
    ids_one,
    ids_two,
    ids_three,
    match_one,
    match_two,
    match_three,
    target_one,
    target_two,
    target_three,
    vertex_weights,
):
    n, groups = lax.axis_size("dev"), lax.axis_size("grp")
    count, width = blocks.shape[0], blocks.shape[1]
    rows = width // 2
    lanes = -(-count // width) * width
    owned = vertex_weights.shape[0]
    slots = count // 4
    per = slots // groups
    chips = n // 2
    across = 1
    while across * across < chips:
        across *= 2
    down = chips // across
    hop_one = max((across - 1) * down, (down - 1) * across, 1)
    hop_two = max(across - 1, down - 1, 1)
    plan_rows = -(-(4 + -(-n * slots // lanes)) // ROWS) * ROWS
    chunks = math.gcd(count, 8)
    code = (per, rows, width)

    def message(*lead):
        return [pltpu.VMEM(lead + code, jnp.int16), pltpu.VMEM(lead + (per, width), jnp.float32)] * 2

    coarse, relative = pl.pallas_call(
        functools.partial(coarsen, n, groups, across),
        in_specs=[SMEM, HBM] + [VMEM] * 8,
        out_specs=(VMEM, VMEM),
        out_shape=(
            jax.ShapeDtypeStruct((count // 8, 2, rows, width), jnp.float32),
            jax.ShapeDtypeStruct((owned // 8, width), jnp.float32),
        ),
        scratch_shapes=[
            pltpu.VMEM(match_one.shape, jnp.int32),
            pltpu.VMEM((count, width, width), jnp.bfloat16),
            pltpu.VMEM((count, width, width), jnp.bfloat16),
            pltpu.VMEM((ROWS, lanes), jnp.int32),
            pltpu.VMEM((n, ROWS, lanes), jnp.int32),
            pltpu.VMEM((groups, ROWS, lanes), jnp.int32),
            pltpu.VMEM((n, owned, width), jnp.float32),
            pltpu.VMEM((owned, width), jnp.float32),
            pltpu.VMEM((groups, owned, width), jnp.float32),
            pltpu.VMEM((plan_rows, lanes), jnp.int32),
            pltpu.SMEM((plan_rows, lanes), jnp.int32),
            pltpu.SMEM((ROWS, lanes), jnp.int32),
            pltpu.VMEM((owned // 8, width), jnp.float32),
            pltpu.VMEM((2 * count + 1, rows, width), jnp.float32),
            *message(groups, 2, hop_one),
            *message(groups, 2, hop_two),
            *message(groups, 2),
            pltpu.VMEM((groups * per + 1, 2, rows, width), jnp.float32),
            pltpu.SemaphoreType.DMA((2, n)),
            pltpu.SemaphoreType.DMA((2, n)),
            pltpu.SemaphoreType.DMA((2, groups)),
            pltpu.SemaphoreType.DMA((2, groups)),
            pltpu.SemaphoreType.DMA((chunks,)),
            pltpu.SemaphoreType.DMA((chunks,)),
            pltpu.SemaphoreType.DMA((groups, 2, hop_one, 2)),
            pltpu.SemaphoreType.DMA((groups, 2, hop_one, 2)),
            pltpu.SemaphoreType.DMA((groups, 2, hop_two, 2)),
            pltpu.SemaphoreType.DMA((groups, 2, hop_two, 2)),
            pltpu.SemaphoreType.DMA((groups, 2, 2)),
            pltpu.SemaphoreType.DMA((groups, 2, 2)),
            pltpu.SemaphoreType.DMA((chunks,)),
            pltpu.SemaphoreType.DMA((2,)),
        ],
        compiler_params=pltpu.CompilerParams(
            collective_id=0, has_side_effects=True, vmem_limit_bytes=63 * 1024 * 1024
        ),
    )(
        ids_one,
        blocks,
        ids_one,
        target_one[None],
        target_two[None],
        target_three[None],
        vertex_weights,
        match_one,
        match_two,
        match_three,
    )
    return coarse.reshape(count // 8, width, width), relative


def solution(mesh):
    both = ("grp", "dev")
    return jax.shard_map(
        per_device,
        mesh=mesh,
        in_specs=(
            P(both, None, None),
            P(None, both),
            P(None, both),
            P(None, both),
            P(),
            P(),
            P(),
            P(both),
            P(both),
            P(both),
            P(both, None),
        ),
        out_specs=(P(both, None, None), P(both, None)),
        check_vma=False,
    )
```

```python
import functools
import math

import jax
import jax.numpy as jnp
from jax import lax
from jax.experimental import pallas as pl
from jax.experimental.pallas import tpu as pltpu
from jax.sharding import PartitionSpec as P

LEVELS = 32767.0
TINY = 1e-30
NT = (((1,), (1,)), ((), ()))
ROWS = 8


def hot(row, rows):
    names = lax.broadcasted_iota(jnp.int32, (rows, row.shape[1]), 0)
    return (names == row).astype(jnp.bfloat16)


def halves(x):
    high = x.astype(jnp.bfloat16)
    low = (x - high.astype(jnp.float32)).astype(jnp.bfloat16)
    return high, low


def project(block, row, col):
    left = hot(row, row.shape[1])
    halfway = jnp.dot(left, block, preferred_element_type=jnp.float32)
    right = hot(col, col.shape[1])
    both = jnp.concatenate([right, right], axis=1)
    split = jnp.concatenate(halves(halfway), axis=1)
    return lax.dot_general(split, both, NT, preferred_element_type=jnp.float32)


def encode(part):
    peak = jnp.maximum(jnp.max(jnp.abs(part), axis=0, keepdims=True), TINY)
    code = jnp.round(part * (LEVELS / peak)).astype(jnp.int32)
    return code.astype(jnp.int16), peak * (1.0 / LEVELS)


def decode(code, scale):
    return code.astype(jnp.int32).astype(jnp.float32) * scale


def lookup(table, index):
    return jnp.take_along_axis(table, index, axis=1, mode="promise_in_bounds")


def fold(weights, row):
    width = row.shape[1]
    place = lax.broadcasted_iota(jnp.int32, (ROWS, width), 0)
    rest = jnp.broadcast_to(weights, (ROWS, width))
    split = jnp.zeros((ROWS, width), jnp.float32)
    for turn in range(3):
        part = rest.astype(jnp.bfloat16).astype(jnp.float32)
        rest = rest - part
        split = jnp.where(place == turn, part, split)
    right = hot(row, width)
    return lax.dot_general(split.astype(jnp.bfloat16), right, NT, preferred_element_type=jnp.float32)


def column(row):
    lanes = row.shape[1]
    return jnp.broadcast_to(row, (lanes, lanes)).T


def latest(match, order):
    return jnp.max(jnp.where(match, order, -1), axis=0, keepdims=True)


def coarsen(
    n,
    groups,
    across,
    ids_smem,
    blocks,
    ids,
    target_one,
    target_two,
    target_three,
    weight,
    match_one,
    match_two,
    match_three,
    coarse,
    relative,
    table,
    own,
    labels,
    land_labels,
    land_far,
    land_weight,
    near_weight,
    land_weight_far,
    plan,
    plan_smem,
    coarse_weight,
    sums,
    out_half,
    out_scale_half,
    land_half,
    land_scale_half,
    out_one,
    out_scale_one,
    land_one,
    land_scale_one,
    out_two,
    out_scale_two,
    land_two,
    land_scale_two,
    out_three,
    out_scale_three,
    land_three,
    land_scale_three,
    sums_three,
    near_send,
    near_recv,
    far_send,
    far_recv,
    half_send,
    half_recv,
    one_send,
    one_recv,
    two_send,
    two_recv,
    three_send,
    three_recv,
    own_sem,
    local,
    free,
):
    me = lax.axis_index("dev")
    group = lax.axis_index("grp")
    core, chip = me % 2, me // 2
    sibling = me + 1 - 2 * core
    chips = n // 2
    down = chips // across
    my_x, my_y = chip % across, chip // across
    count = own.shape[0]
    width = own.shape[2]
    rows = width // 2
    lanes = labels.shape[1]
    per_one, per_two, slots_two = count // n, count // 2 // n, count // 4
    per_three = slots_two // groups
    quarter = match_three.shape[0]
    ring = out_half.shape[0]
    trips = own_sem.shape[0]
    unroll = count // trips
    middle = trips * 3 // 4
    sizes = ((across, down), (down, across))

    def peer(step):
        return lax.rem(me + step, n)

    def source(step):
        return lax.rem(me - step + n, n)

    def far_peer(step):
        return lax.rem(group + step, groups)

    def far_source(step):
        return lax.rem(group - step + groups, groups)

    def remote(src, dst, send, recv, device):
        return pltpu.make_async_remote_copy(
            src_ref=src,
            dst_ref=dst,
            send_sem=send,
            recv_sem=recv,
            device_id=device,
            device_id_type=pl.DeviceIdType.MESH,
        )

    def send_labels(v, here):
        return remote(labels, land_labels.at[here], near_send.at[0, v], near_recv.at[0, here], {"dev": v})

    def send_weight(v, here):
        return remote(weight, land_weight.at[here], near_send.at[1, v], near_recv.at[1, here], {"dev": v})

    def send_labels_far(v, here):
        return remote(labels, land_far.at[here], far_send.at[0, v], far_recv.at[0, here], {"grp": v})

    def send_weight_far(v, here):
        return remote(
            near_weight, land_weight_far.at[here], far_send.at[1, v], far_recv.at[1, here], {"grp": v}
        )

    def own_copy(i):
        part = pl.ds(i * unroll, unroll)
        return pltpu.make_async_copy(blocks.at[part], own.at[part], own_sem.at[i])

    def send_half(i, dx, dy):
        at, r = i % ring, dy * across + dx
        return (
            remote(
                out_half.at[at, r], land_half.at[at, r], half_send.at[at, r, 0], half_recv.at[at, r, 0],
                {"dev": sibling},
            ),
            remote(
                out_scale_half.at[at, r], land_scale_half.at[at, r], half_send.at[at, r, 1],
                half_recv.at[at, r, 1], {"dev": sibling},
            ),
        )

    def chip_at(b, first, second):
        return second * across + first if b == 0 else first * across + second

    def here_of(b):
        return (my_x, my_y) if b == 0 else (my_y, my_x)

    def send_one(i, b, step, turn):
        z, w = sizes[b]
        first, second = here_of(b)
        m = (step - 1) * w + turn
        to = chip_at(b, (first + step) % z, second) * 2 + core
        return (
            remote(
                out_one.at[i, b, m], land_one.at[i, b, m], one_send.at[i, b, m, 0],
                one_recv.at[i, b, m, 0], {"dev": to},
            ),
            remote(
                out_scale_one.at[i, b, m], land_scale_one.at[i, b, m], one_send.at[i, b, m, 1],
                one_recv.at[i, b, m, 1], {"dev": to},
            ),
        )

    def send_two(i, b, turn):
        w = sizes[b][1]
        first, second = here_of(b)
        m = turn - 1
        to = chip_at(b, first, (second + turn) % w) * 2 + core
        return (
            remote(
                out_two.at[i, b, m], land_two.at[i, b, m], two_send.at[i, b, m, 0],
                two_recv.at[i, b, m, 0], {"dev": to},
            ),
            remote(
                out_scale_two.at[i, b, m], land_scale_two.at[i, b, m], two_send.at[i, b, m, 1],
                two_recv.at[i, b, m, 1], {"dev": to},
            ),
        )

    def send_three(i, b, to_group, from_group, from_core):
        device = {"grp": to_group, "dev": chip * 2 + b}
        return (
            remote(
                out_three.at[i, b], land_three.at[from_group, from_core], three_send.at[i, b, 0],
                three_recv.at[from_group, from_core, 0], device,
            ),
            remote(
                out_scale_three.at[i, b], land_scale_three.at[from_group, from_core],
                three_send.at[i, b, 1], three_recv.at[from_group, from_core, 1], device,
            ),
        )

    def chunk_group(i):
        falling = groups - 1 - i
        low = jnp.where(falling > group, falling, falling - 1)
        high = jnp.where(i < group, i, i + 1)
        other = jnp.where(group < groups // 2, low, high)
        return jnp.where(i == groups - 1, group, other)

    for i in range(trips):
        own_copy(i).start()

    barrier = pltpu.get_barrier_semaphore()

    @pl.loop(1, n)
    def _(step):
        pl.semaphore_signal(
            barrier, inc=1, device_id={"dev": peer(step)}, device_id_type=pl.DeviceIdType.MESH
        )

    @pl.loop(1, groups)
    def _(step):
        v = far_peer(step)
        pl.semaphore_signal(
            barrier, inc=1, device_id={"grp": v}, device_id_type=pl.DeviceIdType.MESH
        )
        pl.semaphore_signal(
            barrier, inc=1, device_id={"grp": v, "dev": sibling}, device_id_type=pl.DeviceIdType.MESH
        )

    labels[...] = jnp.zeros(labels.shape, jnp.int32)
    labels[0:2, 0:count] = ids[...]
    labels[2:3, 0:count] = target_one[...]
    labels[3:4, 0 : count // 2] = target_two[...]
    labels[4:5, 0 : count // 4] = target_three[...]
    named = labels[...]
    land_labels[me] = named
    land_far[group] = named

    pl.semaphore_wait(barrier, n - 1 + 2 * (groups - 1))

    @pl.loop(1, n)
    def _(step):
        send_labels(peer(step), me).start()
        send_weight(peer(step), me).start()

    @pl.loop(1, groups)
    def _(step):
        send_labels_far(far_peer(step), group).start()

    for turn in range(4):
        one = match_one[pl.ds(turn, quarter, stride=4), :]
        two = match_two[pl.ds(turn // 2, quarter, stride=2), :]
        table[turn * quarter : (turn + 1) * quarter, :] = lookup(match_three[...], lookup(two, one))

    def mapping(b):
        return table[pl.ds((b % 4) * quarter + b // 4, 1), :]

    none = count
    sums[none] = jnp.zeros(sums.shape[1:], jnp.float32)
    sums_three[groups * per_three] = jnp.zeros(sums_three.shape[1:], jnp.float32)

    def level(i, chained):
        own_copy(i).wait()
        parts = []
        for j in range(unroll):
            k = i * unroll + j
            row, col = mapping(ids_smem[0, k]), mapping(ids_smem[1, k])
            parts.append(project(own[k], row, col))
        for j in range(unroll):
            k = i * unroll + j
            sums[k] = parts[j] + sums[plan_smem[0, k] if chained else none]

    @pl.loop(0, max(middle - 1, 0))
    def _(i):
        level(i, False)

    @pl.loop(1, n)
    def _(step):
        send_labels(source(step), source(step)).wait_recv()
        send_weight(source(step), source(step)).wait_recv()

    @pl.loop(1, groups)
    def _(step):
        send_labels_far(far_source(step), far_source(step)).wait_recv()

    square = (lanes, lanes)
    lane = lax.broadcasted_iota(jnp.int32, (1, lanes), 1)
    order_down = lax.broadcasted_iota(jnp.int32, square, 0)
    order_across = lax.broadcasted_iota(jnp.int32, square, 1)

    def slots_of(mine):
        first = mine[2:3, :]
        spread = jnp.broadcast_to(first, mine.shape)
        second = jnp.zeros((1, lanes), jnp.int32)
        for o in range(n):
            second = jnp.where(lane // per_one == o, lookup(land_labels[o], spread)[3:4, :], second)
        return first // per_two * slots_two + second

    slot_own = slots_of(named)
    down_own = column(slot_own)
    before = latest((down_own == slot_own) & (order_down < order_across), order_down)
    plan[0:1, :] = jnp.where(before < 0, none, before)
    blocks_of_slots = -(-n * slots_two // lanes)
    for part in range(blocks_of_slots):
        name = order_across + part * lanes
        last = latest(down_own == name, order_down)
        plan[1 + part : 2 + part, :] = jnp.where(last < 0, none, last)
    total = groups * per_three
    pick = jnp.broadcast_to(group * per_three + lane % per_three, (ROWS, lanes))
    third = jnp.full((1, lanes), -1, jnp.int32)
    for u in range(groups):
        third = jnp.where(lane // per_three == u, lookup(land_far[u], pick)[4:5, :], third)
    down_third = column(third)

    def rank(k):
        return (group - k // per_three - 1 + groups) % groups * per_three + k % per_three

    rank_down, rank_across = rank(order_down), rank(order_across)
    real = order_down < total
    before = latest(real & (down_third == third) & (rank_down < rank_across), rank_down)
    last = latest(real & (down_third == order_across), rank_down)
    third_row = 1 + blocks_of_slots
    plan[third_row : third_row + 1, :] = jnp.where(before < 0, total, before)
    plan[third_row + 1 : third_row + 2, :] = jnp.where(last < 0, total, last)
    rest = plan.shape[0] - third_row - 2
    if rest:
        plan[third_row + 2 :, :] = jnp.zeros((rest, lanes), jnp.int32)
    to_smem = pltpu.make_async_copy(plan, plan_smem, local.at[1])
    to_smem.start()

    held = weight[...]
    for step in range(1, n):
        held = held + land_weight[peer(step)]
    near_weight[...] = held

    @pl.loop(1, groups)
    def _(step):
        send_weight_far(far_peer(step), group).start()

    @pl.loop(max(middle - 1, 0), middle)
    def _(i):
        level(i, False)

    to_smem.wait()

    @pl.loop(0, middle)
    def _(i):
        for j in range(unroll):
            k = i * unroll + j
            sums[k] = sums[k] + sums[plan_smem[0, k]]

    @pl.loop(middle, trips)
    def _(i):
        level(i, True)

    def from_own(to_chip, b, i, j, h):
        slot = (to_chip * 2 + b) * slots_two + chunk_group(i) * per_three + j
        spot = plan_smem[1 + slot // lanes, slot % lanes]
        return sums[spot, pl.ds(pl.multiple_of(h * rows, rows), rows), :]

    def held_here(b, i, dx, dy):
        to = (my_y + dy) % down * across + (my_x + dx) % across
        at, r = i % ring, dy * across + dx
        parts = []
        for j in range(per_three):
            m = b * per_three + j
            part = decode(land_half[at, r, m], land_scale_half[at, r, m : m + 1, :])
            parts.append(part + from_own(to, b, i, j, core))
        return parts

    places = [(dx, dy) for dy in range(down) for dx in range(across)]
    places.sort(key=lambda p: (p[0] == 0) + (p[1] == 0))

    def spread(i):
        if ring < groups:

            @pl.when(i >= ring)
            def _():
                pl.semaphore_wait(free, 1)
                for dx, dy in places:
                    sent(send_half(i, dx, dy))

        for dx, dy in places:
            to = (my_y + dy) % down * across + (my_x + dx) % across
            at, r = i % ring, dy * across + dx
            parts = [from_own(to, b, i, j, 1 - core) for b in range(2) for j in range(per_three)]
            pack(parts, out_half.at[at, r], out_scale_half.at[at, r])
            start(send_half(i, dx, dy))

    def release(i):
        if ring < groups:

            @pl.when(i < groups - ring)
            def _():
                pl.semaphore_signal(
                    free, inc=1, device_id={"dev": sibling}, device_id_type=pl.DeviceIdType.MESH
                )

    def pack(parts, codes, scales):
        for j, part in enumerate(parts):
            code, scale = encode(part)
            codes[j] = code
            scales[j : j + 1, :] = scale

    def start(copies):
        for copy in copies:
            copy.start()

    def arrive(copies):
        for copy in copies:
            copy.wait_recv()

    def sent(copies):
        for copy in copies:
            copy.wait_send()

    def offset(b, first, second):
        return (first, second) if b == 0 else (second, first)

    def turns(b):
        w = sizes[b][1]
        return [*range(1, w), 0]

    def first_hop(i):
        here = set()
        for spot in range(max(across, down)):
            for b in range(2):
                z, w = sizes[b]
                if spot >= w:
                    continue
                turn = turns(b)[spot]
                for step in range(1, z):
                    m = (step - 1) * w + turn
                    place = offset(b, step, turn)
                    if place not in here:
                        here.add(place)
                        arrive(send_half(i, *place))
                    parts = held_here(b, i, *place)
                    pack(parts, out_one.at[i, b, m], out_scale_one.at[i, b, m])
                    start(send_one(i, b, step, turn))

    def with_first(parts, i, b, turn):
        z, w = sizes[b]
        for step in range(1, z):
            m = (step - 1) * w + turn
            arrive(send_one(i, b, step, turn))
            parts = [
                p + decode(land_one[i, b, m, j], land_scale_one[i, b, m, j : j + 1, :])
                for j, p in enumerate(parts)
            ]
        return parts

    def second_hop(i):
        for b in range(2):
            w = sizes[b][1]
            for turn in range(1, w):
                parts = held_here(b, i, *offset(b, 0, turn))
                parts = with_first(parts, i, b, turn)
                pack(parts, out_two.at[i, b, turn - 1], out_scale_two.at[i, b, turn - 1])
                start(send_two(i, b, turn))

    def reduced(i):
        arrive(send_half(i, 0, 0))
        for b in range(2):
            w = sizes[b][1]
            parts = held_here(b, i, 0, 0)
            parts = with_first(parts, i, b, 0)
            for turn in range(1, w):
                arrive(send_two(i, b, turn))
                parts = [
                    p + decode(land_two[i, b, turn - 1, j], land_scale_two[i, b, turn - 1, j : j + 1, :])
                    for j, p in enumerate(parts)
                ]
            pack(parts, out_three.at[i, b], out_scale_three.at[i, b])
        release(i)

    def third_hop(i):
        reduced(i)
        for b in range(2):
            start(send_three(i, b, chunk_group(i), group, core))

    spread(0)

    @pl.loop(0, groups)
    def _(i):
        first_hop(i)

        @pl.when(i > 0)
        def _():
            third_hop(i - 1)

        @pl.when(i + 1 < groups)
        def _():
            spread(i + 1)

        second_hop(i)

    owned = weight.shape[0]
    start_row = (group * n + me) * (owned // 4)
    for e in range(owned // 8):
        folded = jnp.zeros((ROWS, width), jnp.float32)
        for f in range(8 * e, 8 * e + 8):
            row = table[pl.ds(f % 4 * quarter + start_row + f // 4, 1), :]
            folded = folded + fold(weight[f : f + 1, :], row)
        coarse_weight[e : e + 1, :] = jnp.sum(folded, axis=0, keepdims=True)
    held = near_weight[...]
    for step in range(1, groups):
        send_weight_far(far_source(step), far_source(step)).wait_recv()
        held = held + land_weight_far[far_source(step)]
    whole = jnp.sum(jnp.sum(held, axis=0, keepdims=True), axis=1, keepdims=True)
    vertices = relative.shape[0] * n * groups * relative.shape[1]
    relative[...] = coarse_weight[...] * vertices / whole

    end = groups - 1
    reduced(end)
    start(send_three(end, 1 - core, group, group, core))

    def take(codes, scales, at, h, u):
        for j in range(per_three):
            part = decode(codes[j], scales[j : j + 1, :])
            sums_three[at + j, h] = part + sums_three[plan_smem[third_row, u * per_three + j], h]

    @pl.loop(1, groups)
    def _(step):
        u = far_source(step)
        for h in range(2):
            arrive(send_three(0, h, u, u, h))
            take(land_three.at[u, h], land_scale_three.at[u, h], (step - 1) * per_three, h, u)

    take(out_three.at[end, core], out_scale_three.at[end, core], end * per_three, core, group)
    other = 1 - core
    arrive(send_three(end, other, group, group, other))
    take(land_three.at[group, other], land_scale_three.at[group, other], end * per_three, other, group)

    @pl.loop(0, coarse.shape[0])
    def _(slot):
        coarse[slot] = sums_three[plan_smem[third_row + 1, slot]]

    @pl.loop(1, n)
    def _(step):
        send_labels(peer(step), me).wait_send()
        send_weight(peer(step), me).wait_send()

    @pl.loop(1, groups)
    def _(step):
        send_labels_far(far_peer(step), group).wait_send()
        send_weight_far(far_peer(step), group).wait_send()

    @pl.loop(groups - ring, groups)
    def _(i):
        for dx, dy in places:
            sent(send_half(i, dx, dy))

    @pl.loop(0, groups)
    def _(i):
        for b in range(2):
            z, w = sizes[b]
            for step in range(1, z):
                for turn in range(w):
                    sent(send_one(i, b, step, turn))
            for turn in range(1, w):
                sent(send_two(i, b, turn))

    @pl.loop(0, groups - 1)
    def _(i):
        for b in range(2):
            sent(send_three(i, b, group, group, core))

    sent(send_three(end, 1 - core, group, group, core))


SMEM = pl.BlockSpec(memory_space=pltpu.SMEM)
VMEM = pl.BlockSpec(memory_space=pltpu.VMEM)
HBM = pl.BlockSpec(memory_space=pl.ANY)
VMEM_BYTES = 67_043_328


def per_device(
    blocks,
    ids_one,
    ids_two,
    ids_three,
    match_one,
    match_two,
    match_three,
    target_one,
    target_two,
    target_three,
    vertex_weights,
):
    n, groups = lax.axis_size("dev"), lax.axis_size("grp")
    count, width = blocks.shape[0], blocks.shape[1]
    rows = width // 2
    lanes = -(-count // width) * width
    owned = vertex_weights.shape[0]
    slots = count // 4
    per = slots // groups
    chips = n // 2
    across = 1
    while across * across < chips:
        across *= 2
    down = chips // across
    hop_one = max((across - 1) * down, (down - 1) * across, 1)
    hop_two = max(across - 1, down - 1, 1)
    plan_rows = -(-(3 + -(-n * slots // lanes)) // ROWS) * ROWS
    half_bytes = groups * chips * 4 * per * rows * width * 2
    ring = groups if half_bytes <= VMEM_BYTES // 4 else 2

    def message(*lead, per=per):
        return [
            pltpu.VMEM(lead + (per, rows, width), jnp.int16),
            pltpu.VMEM(lead + (per, width), jnp.float32),
        ] * 2

    coarse, relative = pl.pallas_call(
        functools.partial(coarsen, n, groups, across),
        in_specs=[SMEM, HBM] + [VMEM] * 8,
        out_specs=(VMEM, VMEM),
        out_shape=(
            jax.ShapeDtypeStruct((count // 8, 2, rows, width), jnp.float32),
            jax.ShapeDtypeStruct((owned // 8, width), jnp.float32),
        ),
        scratch_shapes=[
            pltpu.VMEM(match_one.shape, jnp.int32),
            pltpu.VMEM((count, width, width), jnp.bfloat16),
            pltpu.VMEM((ROWS, lanes), jnp.int32),
            pltpu.VMEM((n, ROWS, lanes), jnp.int32),
            pltpu.VMEM((groups, ROWS, lanes), jnp.int32),
            pltpu.VMEM((n, owned, width), jnp.float32),
            pltpu.VMEM((owned, width), jnp.float32),
            pltpu.VMEM((groups, owned, width), jnp.float32),
            pltpu.VMEM((plan_rows, lanes), jnp.int32),
            pltpu.SMEM((plan_rows, lanes), jnp.int32),
            pltpu.VMEM((owned // 8, width), jnp.float32),
            pltpu.VMEM((count + 1, width, width), jnp.float32),
            *message(ring, chips, per=2 * per),
            *message(groups, 2, hop_one),
            *message(groups, 2, hop_two),
            *message(groups, 2),
            pltpu.VMEM((groups * per + 1, 2, rows, width), jnp.float32),
            pltpu.SemaphoreType.DMA((2, n)),
            pltpu.SemaphoreType.DMA((2, n)),
            pltpu.SemaphoreType.DMA((2, groups)),
            pltpu.SemaphoreType.DMA((2, groups)),
            pltpu.SemaphoreType.DMA((ring, chips, 2)),
            pltpu.SemaphoreType.DMA((ring, chips, 2)),
            pltpu.SemaphoreType.DMA((groups, 2, hop_one, 2)),
            pltpu.SemaphoreType.DMA((groups, 2, hop_one, 2)),
            pltpu.SemaphoreType.DMA((groups, 2, hop_two, 2)),
            pltpu.SemaphoreType.DMA((groups, 2, hop_two, 2)),
            pltpu.SemaphoreType.DMA((groups, 2, 2)),
            pltpu.SemaphoreType.DMA((groups, 2, 2)),
            pltpu.SemaphoreType.DMA((count // math.gcd(count, 16),)),
            pltpu.SemaphoreType.DMA((2,)),
            pltpu.SemaphoreType.REGULAR,
        ],
        compiler_params=pltpu.CompilerParams(
            collective_id=0,
            has_side_effects=True,
            vmem_limit_bytes=VMEM_BYTES,
        ),
    )(
        ids_one,
        blocks,
        ids_one,
        target_one[None],
        target_two[None],
        target_three[None],
        vertex_weights,
        match_one,
        match_two,
        match_three,
    )
    return coarse.reshape(count // 8, width, width), relative


def solution(mesh):
    both = ("grp", "dev")
    return jax.shard_map(
        per_device,
        mesh=mesh,
        in_specs=(
            P(both, None, None),
            P(None, both),
            P(None, both),
            P(None, both),
            P(),
            P(),
            P(),
            P(both),
            P(both),
            P(both),
            P(both, None),
        ),
        out_specs=(P(both, None, None), P(both, None)),
        check_vma=False,
    )
```

```python
import functools
import math

import jax
import jax.numpy as jnp
from jax import lax
from jax.experimental import pallas as pl
from jax.experimental.pallas import tpu as pltpu
from jax.sharding import PartitionSpec as P

LEVELS = 32767.0
TINY = 1e-30
NT = (((1,), (1,)), ((), ()))
ROWS = 8


def hot(row, rows):
    names = lax.broadcasted_iota(jnp.int32, (rows, row.shape[1]), 0)
    return (names == row).astype(jnp.bfloat16)


def halves(x):
    high = x.astype(jnp.bfloat16)
    low = (x - high.astype(jnp.float32)).astype(jnp.bfloat16)
    return high, low


def project(block, row, col):
    left = hot(row, row.shape[1])
    halfway = jnp.dot(left, block, preferred_element_type=jnp.float32)
    right = hot(col, col.shape[1])
    both = jnp.concatenate([right, right], axis=1)
    split = jnp.concatenate(halves(halfway), axis=1)
    return lax.dot_general(split, both, NT, preferred_element_type=jnp.float32)


def encode(part):
    peak = jnp.maximum(jnp.max(jnp.abs(part), axis=0, keepdims=True), TINY)
    code = jnp.round(part * (LEVELS / peak)).astype(jnp.int32)
    return code.astype(jnp.int16), peak * (1.0 / LEVELS)


def decode(code, scale):
    return code.astype(jnp.int32).astype(jnp.float32) * scale


def lookup(table, index):
    return jnp.take_along_axis(table, index, axis=1, mode="promise_in_bounds")


def fold(weights, row):
    width = row.shape[1]
    place = lax.broadcasted_iota(jnp.int32, (ROWS, width), 0)
    rest = jnp.broadcast_to(weights, (ROWS, width))
    split = jnp.zeros((ROWS, width), jnp.float32)
    for turn in range(3):
        part = rest.astype(jnp.bfloat16).astype(jnp.float32)
        rest = rest - part
        split = jnp.where(place == turn, part, split)
    right = hot(row, width)
    return lax.dot_general(split.astype(jnp.bfloat16), right, NT, preferred_element_type=jnp.float32)


def column(row):
    lanes = row.shape[1]
    return jnp.broadcast_to(row, (lanes, lanes)).T


def latest(match, order):
    return jnp.max(jnp.where(match, order, -1), axis=0, keepdims=True)


def coarsen(
    n,
    groups,
    across,
    ids_smem,
    blocks,
    ids,
    target_one,
    target_two,
    target_three,
    weight,
    match_one,
    match_two,
    match_three,
    coarse,
    relative,
    table,
    own,
    labels,
    land_labels,
    land_far,
    land_weight,
    near_weight,
    land_weight_far,
    plan,
    plan_smem,
    plan_third,
    third_smem,
    coarse_weight,
    sums,
    out_half,
    out_scale_half,
    land_half,
    land_scale_half,
    out_one,
    out_scale_one,
    land_one,
    land_scale_one,
    out_two,
    out_scale_two,
    land_two,
    land_scale_two,
    out_three,
    out_scale_three,
    land_three,
    land_scale_three,
    sums_three,
    bulk,
    bulk_half,
    near_send,
    near_recv,
    far_send,
    far_recv,
    half_send,
    half_recv,
    one_send,
    one_recv,
    two_send,
    two_recv,
    three_send,
    three_recv,
    own_sem,
    local,
    free,
):
    me = lax.axis_index("dev")
    group = lax.axis_index("grp")
    core, chip = me % 2, me // 2
    sibling = me + 1 - 2 * core
    chips = n // 2
    down = chips // across
    my_x, my_y = chip % across, chip // across
    count = own.shape[0]
    width = own.shape[2]
    rows = width // 2
    lanes = labels.shape[1]
    per_one, per_two, slots_two = count // n, count // 2 // n, count // 4
    per_three = slots_two // groups
    quarter = match_three.shape[0]
    ring = out_half.shape[0]
    trips = own_sem.shape[0]
    unroll = count // trips
    middle = trips * 3 // 4
    sizes = ((across, down), (down, across))

    def peer(step):
        return lax.rem(me + step, n)

    def source(step):
        return lax.rem(me - step + n, n)

    def far_peer(step):
        return lax.rem(group + step, groups)

    def far_source(step):
        return lax.rem(group - step + groups, groups)

    def remote(src, dst, send, recv, device):
        return pltpu.make_async_remote_copy(
            src_ref=src,
            dst_ref=dst,
            send_sem=send,
            recv_sem=recv,
            device_id=device,
            device_id_type=pl.DeviceIdType.MESH,
        )

    def settle(ref, sem):
        pltpu.make_async_copy(ref, ref, sem).wait()

    def send_labels(v, here):
        return remote(labels, land_labels.at[here], near_send.at[0], near_recv.at[0], {"dev": v})

    def send_weight(v, here):
        return remote(weight, land_weight.at[here], near_send.at[1], near_recv.at[1], {"dev": v})

    def send_labels_far(v, here):
        return remote(labels, land_far.at[here], far_send.at[0], far_recv.at[0], {"grp": v})

    def send_weight_far(v, here):
        return remote(
            near_weight, land_weight_far.at[here], far_send.at[1], far_recv.at[1], {"grp": v}
        )

    def own_copy(i):
        part = pl.ds(i * unroll, unroll)
        return pltpu.make_async_copy(blocks.at[part], own.at[part], own_sem.at[i])

    def send_half(i, dx, dy):
        at, r = i % ring, dy * across + dx
        return (
            remote(
                out_half.at[at, r], land_half.at[at, r], half_send.at[at, 0], half_recv.at[at, r],
                {"dev": sibling},
            ),
            remote(
                out_scale_half.at[at, r], land_scale_half.at[at, r], half_send.at[at, 1],
                half_recv.at[at, r], {"dev": sibling},
            ),
        )

    def chip_at(b, first, second):
        return second * across + first if b == 0 else first * across + second

    def here_of(b):
        return (my_x, my_y) if b == 0 else (my_y, my_x)

    def send_one(i, b, step, turn):
        z, w = sizes[b]
        first, second = here_of(b)
        m = (step - 1) * w + turn
        to = chip_at(b, (first + step) % z, second) * 2 + core
        return (
            remote(
                out_one.at[i, b, m], land_one.at[i, b, m], one_send.at[b, 0],
                one_recv.at[i, b, m], {"dev": to},
            ),
            remote(
                out_scale_one.at[i, b, m], land_scale_one.at[i, b, m], one_send.at[b, 1],
                one_recv.at[i, b, m], {"dev": to},
            ),
        )

    def send_two(i, b, turn):
        w = sizes[b][1]
        first, second = here_of(b)
        m = turn - 1
        to = chip_at(b, first, (second + turn) % w) * 2 + core
        return (
            remote(
                out_two.at[i, b, m], land_two.at[i, b, m], two_send.at[b, 0],
                two_recv.at[i, b, m], {"dev": to},
            ),
            remote(
                out_scale_two.at[i, b, m], land_scale_two.at[i, b, m], two_send.at[b, 1],
                two_recv.at[i, b, m], {"dev": to},
            ),
        )

    def send_three(i, b, to_group, from_group, from_core):
        device = {"grp": to_group, "dev": chip * 2 + b}
        return (
            remote(
                out_three.at[i * 2 + b], land_three.at[from_group, from_core], three_send.at[0],
                three_recv.at[from_group, from_core], device,
            ),
            remote(
                out_scale_three.at[i * 2 + b], land_scale_three.at[from_group, from_core],
                three_send.at[1], three_recv.at[from_group, from_core], device,
            ),
        )

    def chunk_group(i):
        falling = groups - 1 - i
        low = jnp.where(falling > group, falling, falling - 1)
        high = jnp.where(i < group, i, i + 1)
        other = jnp.where(group < groups // 2, low, high)
        return jnp.where(i == groups - 1, group, other)

    for i in range(trips):
        own_copy(i).start()

    barrier = pltpu.get_barrier_semaphore()

    @pl.loop(1, n)
    def _(step):
        pl.semaphore_signal(
            barrier, inc=1, device_id={"dev": peer(step)}, device_id_type=pl.DeviceIdType.MESH
        )

    @pl.loop(1, groups)
    def _(step):
        v = far_peer(step)
        pl.semaphore_signal(
            barrier, inc=1, device_id={"grp": v}, device_id_type=pl.DeviceIdType.MESH
        )
        pl.semaphore_signal(
            barrier, inc=1, device_id={"grp": v, "dev": sibling}, device_id_type=pl.DeviceIdType.MESH
        )

    labels[...] = jnp.zeros(labels.shape, jnp.int32)
    labels[0:2, 0:count] = ids[...]
    labels[2:3, 0:count] = target_one[...]
    labels[3:4, 0 : count // 2] = target_two[...]
    labels[4:5, 0 : count // 4] = target_three[...]
    named = labels[...]
    land_labels[me] = named
    land_far[group] = named

    pl.semaphore_wait(barrier, n - 1 + 2 * (groups - 1))

    @pl.loop(1, n)
    def _(step):
        send_labels(peer(step), me).start()
        send_weight(peer(step), me).start()

    @pl.loop(1, groups)
    def _(step):
        send_labels_far(far_peer(step), group).start()

    for turn in range(4):
        one = match_one[pl.ds(turn, quarter, stride=4), :]
        two = match_two[pl.ds(turn // 2, quarter, stride=2), :]
        table[turn * quarter : (turn + 1) * quarter, :] = lookup(match_three[...], lookup(two, one))

    def mapping(b):
        return table[pl.ds((b % 4) * quarter + b // 4, 1), :]

    none = count
    sums[none] = jnp.zeros(sums.shape[1:], jnp.float32)
    sums_three[groups * per_three] = jnp.zeros(sums_three.shape[1:], jnp.float32)

    def level(i, chained):
        own_copy(i).wait()
        parts = []
        for j in range(unroll):
            k = i * unroll + j
            row, col = mapping(ids_smem[0, k]), mapping(ids_smem[1, k])
            parts.append(project(own[k], row, col))
        for j in range(unroll):
            k = i * unroll + j
            sums[k] = parts[j] + sums[plan_smem[0, k] if chained else none]

    @pl.loop(0, max(middle - 1, 0))
    def _(i):
        level(i, False)

    settle(land_labels.at[pl.ds(0, n - 1)], near_recv.at[0])

    square = (lanes, lanes)
    lane = lax.broadcasted_iota(jnp.int32, (1, lanes), 1)
    order_down = lax.broadcasted_iota(jnp.int32, square, 0)
    order_across = lax.broadcasted_iota(jnp.int32, square, 1)

    def slots_of(mine):
        first = mine[2:3, :]
        spread = jnp.broadcast_to(first, mine.shape)
        second = jnp.zeros((1, lanes), jnp.int32)
        for o in range(n):
            second = jnp.where(lane // per_one == o, lookup(land_labels[o], spread)[3:4, :], second)
        return first // per_two * slots_two + second

    slot_own = slots_of(named)
    down_own = column(slot_own)
    before = latest((down_own == slot_own) & (order_down < order_across), order_down)
    plan[0:1, :] = jnp.where(before < 0, none, before)
    blocks_of_slots = -(-n * slots_two // lanes)
    for part in range(blocks_of_slots):
        name = order_across + part * lanes
        last = latest(down_own == name, order_down)
        plan[1 + part : 2 + part, :] = jnp.where(last < 0, none, last)
    rest = plan.shape[0] - 1 - blocks_of_slots
    if rest:
        plan[1 + blocks_of_slots :, :] = jnp.zeros((rest, lanes), jnp.int32)
    to_smem = pltpu.make_async_copy(plan, plan_smem, local.at[1])
    to_smem.start()

    @pl.loop(max(middle - 1, 0), middle)
    def _(i):
        level(i, False)

    to_smem.wait()

    @pl.loop(0, middle)
    def _(i):
        for j in range(unroll):
            k = i * unroll + j
            sums[k] = sums[k] + sums[plan_smem[0, k]]

    @pl.loop(middle, trips)
    def _(i):
        level(i, True)

    def from_own(to_chip, b, i, j, h):
        slot = (to_chip * 2 + b) * slots_two + chunk_group(i) * per_three + j
        spot = plan_smem[1 + slot // lanes, slot % lanes]
        return sums[spot, pl.ds(pl.multiple_of(h * rows, rows), rows), :]

    def held_here(b, i, dx, dy):
        to = (my_y + dy) % down * across + (my_x + dx) % across
        at, r = i % ring, dy * across + dx
        parts = []
        for j in range(per_three):
            m = b * per_three + j
            part = decode(land_half[at, r, m], land_scale_half[at, r, m : m + 1, :])
            parts.append(part + from_own(to, b, i, j, core))
        return parts

    places = [(dx, dy) for dy in range(down) for dx in range(across)]
    places.sort(key=lambda p: (p[0] == 0) + (p[1] == 0))

    def spread(i):
        if ring < groups:

            @pl.when(i >= ring)
            def _():
                pl.semaphore_wait(free, 1)
                settle(out_half.at[i % ring], half_send.at[i % ring, 0])
                settle(out_scale_half.at[i % ring], half_send.at[i % ring, 1])

        for dx, dy in places:
            to = (my_y + dy) % down * across + (my_x + dx) % across
            at, r = i % ring, dy * across + dx
            parts = [from_own(to, b, i, j, 1 - core) for b in range(2) for j in range(per_three)]
            pack(parts, out_half.at[at, r], out_scale_half.at[at, r])
            start(send_half(i, dx, dy))

    def release(i):
        if ring < groups:

            @pl.when(i < groups - ring)
            def _():
                pl.semaphore_signal(
                    free, inc=1, device_id={"dev": sibling}, device_id_type=pl.DeviceIdType.MESH
                )

    def pack(parts, codes, scales):
        for j, part in enumerate(parts):
            code, scale = encode(part)
            codes[j] = code
            scales[j : j + 1, :] = scale

    def start(copies):
        for copy in copies:
            copy.start()

    def offset(b, first, second):
        return (first, second) if b == 0 else (second, first)

    def turns(b):
        w = sizes[b][1]
        return [*range(1, w), 0]

    def first_hop(i):
        here = set()
        for spot in range(max(across, down)):
            for b in range(2):
                z, w = sizes[b]
                if spot >= w:
                    continue
                turn = turns(b)[spot]
                for step in range(1, z):
                    m = (step - 1) * w + turn
                    place = offset(b, step, turn)
                    if place not in here:
                        here.add(place)
                        settle(bulk_half, half_recv.at[i % ring, place[1] * across + place[0]])
                    parts = held_here(b, i, *place)
                    pack(parts, out_one.at[i, b, m], out_scale_one.at[i, b, m])
                    start(send_one(i, b, step, turn))

    def with_first(parts, i, b, turn):
        z, w = sizes[b]
        for step in range(1, z):
            m = (step - 1) * w + turn
            settle(bulk, one_recv.at[i, b, m])
            parts = [
                p + decode(land_one[i, b, m, j], land_scale_one[i, b, m, j : j + 1, :])
                for j, p in enumerate(parts)
            ]
        return parts

    def second_hop(i):
        for b in range(2):
            w = sizes[b][1]
            for turn in range(1, w):
                parts = held_here(b, i, *offset(b, 0, turn))
                parts = with_first(parts, i, b, turn)
                pack(parts, out_two.at[i, b, turn - 1], out_scale_two.at[i, b, turn - 1])
                start(send_two(i, b, turn))

    def reduced(i):
        settle(bulk_half, half_recv.at[i % ring, 0])
        for b in range(2):
            w = sizes[b][1]
            parts = held_here(b, i, 0, 0)
            parts = with_first(parts, i, b, 0)
            for turn in range(1, w):
                settle(bulk, two_recv.at[i, b, turn - 1])
                parts = [
                    p + decode(land_two[i, b, turn - 1, j], land_scale_two[i, b, turn - 1, j : j + 1, :])
                    for j, p in enumerate(parts)
                ]
            pack(parts, out_three.at[i * 2 + b], out_scale_three.at[i * 2 + b])
        release(i)

    def third_hop(i):
        reduced(i)
        for b in range(2):
            start(send_three(i, b, chunk_group(i), group, core))

    spread(0)

    settle(land_far.at[pl.ds(0, groups - 1)], far_recv.at[0])

    total = groups * per_three
    pick = jnp.broadcast_to(group * per_three + lane % per_three, (ROWS, lanes))
    third = jnp.full((1, lanes), -1, jnp.int32)
    for u in range(groups):
        third = jnp.where(lane // per_three == u, lookup(land_far[u], pick)[4:5, :], third)
    down_third = column(third)

    def rank(k):
        return (group - k // per_three - 1 + groups) % groups * per_three + k % per_three

    rank_down, rank_across = rank(order_down), rank(order_across)
    real = order_down < total
    before = latest(real & (down_third == third) & (rank_down < rank_across), rank_down)
    last = latest(real & (down_third == order_across), rank_down)
    plan_third[0:1, :] = jnp.where(before < 0, total, before)
    plan_third[1:2, :] = jnp.where(last < 0, total, last)
    plan_third[2:, :] = jnp.zeros((plan_third.shape[0] - 2, lanes), jnp.int32)
    third_to_smem = pltpu.make_async_copy(plan_third, third_smem, local.at[0])
    third_to_smem.start()

    settle(land_weight.at[pl.ds(0, n - 1)], near_recv.at[1])

    held = weight[...]
    for step in range(1, n):
        held = held + land_weight[peer(step)]
    near_weight[...] = held

    @pl.loop(1, groups)
    def _(step):
        send_weight_far(far_peer(step), group).start()

    @pl.loop(0, groups)
    def _(i):
        first_hop(i)

        @pl.when(i > 0)
        def _():
            third_hop(i - 1)

        @pl.when(i + 1 < groups)
        def _():
            spread(i + 1)

        second_hop(i)

    owned = weight.shape[0]
    start_row = (group * n + me) * (owned // 4)
    for e in range(owned // 8):
        folded = jnp.zeros((ROWS, width), jnp.float32)
        for f in range(8 * e, 8 * e + 8):
            row = table[pl.ds(f % 4 * quarter + start_row + f // 4, 1), :]
            folded = folded + fold(weight[f : f + 1, :], row)
        coarse_weight[e : e + 1, :] = jnp.sum(folded, axis=0, keepdims=True)
    held = near_weight[...]
    settle(land_weight_far.at[pl.ds(0, groups - 1)], far_recv.at[1])
    for step in range(1, groups):
        held = held + land_weight_far[far_source(step)]
    whole = jnp.sum(jnp.sum(held, axis=0, keepdims=True), axis=1, keepdims=True)
    vertices = relative.shape[0] * n * groups * relative.shape[1]
    relative[...] = coarse_weight[...] * vertices / whole

    third_to_smem.wait()
    end = groups - 1
    reduced(end)
    start(send_three(end, 1 - core, group, group, core))

    def take(codes, scales, at, h, u):
        for j in range(per_three):
            part = decode(codes[j], scales[j : j + 1, :])
            sums_three[at + j, h] = part + sums_three[third_smem[0, u * per_three + j], h]

    @pl.loop(1, groups)
    def _(step):
        u = far_source(step)
        for h in range(2):
            settle(bulk, three_recv.at[u, h])
            take(land_three.at[u, h], land_scale_three.at[u, h], (step - 1) * per_three, h, u)

    take(out_three.at[end * 2 + core], out_scale_three.at[end * 2 + core], end * per_three, core, group)
    other = 1 - core
    settle(bulk, three_recv.at[group, other])
    take(land_three.at[group, other], land_scale_three.at[group, other], end * per_three, other, group)

    @pl.loop(0, coarse.shape[0])
    def _(slot):
        coarse[slot] = sums_three[third_smem[1, slot]]

    settle(land_labels.at[pl.ds(0, n - 1)], near_send.at[0])
    settle(land_weight.at[pl.ds(0, n - 1)], near_send.at[1])
    settle(land_far.at[pl.ds(0, groups - 1)], far_send.at[0])
    settle(land_weight_far.at[pl.ds(0, groups - 1)], far_send.at[1])
    for at in range(ring):
        settle(out_half.at[at], half_send.at[at, 0])
        settle(out_scale_half.at[at], half_send.at[at, 1])
    for b in range(2):
        z, w = sizes[b]
        some, few = pl.ds(0, (z - 1) * w), pl.ds(0, w - 1)
        settle(out_one.at[pl.ds(0, groups), b, some], one_send.at[b, 0])
        settle(out_scale_one.at[pl.ds(0, groups), b, some], one_send.at[b, 1])
        settle(out_two.at[pl.ds(0, groups), b, few], two_send.at[b, 0])
        settle(out_scale_two.at[pl.ds(0, groups), b, few], two_send.at[b, 1])
    settle(out_three.at[pl.ds(0, 2 * groups - 1)], three_send.at[0])
    settle(out_scale_three.at[pl.ds(0, 2 * groups - 1)], three_send.at[1])


def hand_on(coarse_in, relative_in, coarse, relative, blocks, row, arrive, leave):
    pieces = arrive.shape[0] - 1
    size = blocks.shape[0] // pieces
    moves = [(coarse_in, blocks, coarse, pl.ds(i * size, size)) for i in range(pieces)]
    moves.append((relative_in, row, relative, pl.ds(0, row.shape[0])))
    ins = [pltpu.make_async_copy(a.at[p], v.at[p], arrive.at[i]) for i, (a, v, _, p) in enumerate(moves)]
    outs = [pltpu.make_async_copy(v.at[p], b.at[p], leave.at[i]) for i, (_, v, b, p) in enumerate(moves)]
    for copy in ins:
        copy.start()
    for first, second in zip(ins, outs):
        first.wait()
        second.start()
    for copy in outs:
        copy.wait()


SMEM = pl.BlockSpec(memory_space=pltpu.SMEM)
VMEM = pl.BlockSpec(memory_space=pltpu.VMEM)
HBM = pl.BlockSpec(memory_space=pl.ANY)
VMEM_BYTES = 67_043_328


def per_device(
    blocks,
    ids_one,
    ids_two,
    ids_three,
    match_one,
    match_two,
    match_three,
    target_one,
    target_two,
    target_three,
    vertex_weights,
):
    n, groups = lax.axis_size("dev"), lax.axis_size("grp")
    count, width = blocks.shape[0], blocks.shape[1]
    rows = width // 2
    lanes = -(-count // width) * width
    owned = vertex_weights.shape[0]
    slots = count // 4
    per = slots // groups
    chips = n // 2
    across = 1
    while across * across < chips:
        across *= 2
    down = chips // across
    hop_one = max((across - 1) * down, (down - 1) * across, 1)
    hop_two = max(across - 1, down - 1, 1)
    plan_rows = -(-(1 + -(-n * slots // lanes)) // ROWS) * ROWS
    half_bytes = groups * chips * 4 * per * rows * width * 2
    ring = groups if half_bytes <= VMEM_BYTES // 4 else 2

    def message(*lead, per=per):
        return [
            pltpu.VMEM(lead + (per, rows, width), jnp.int16),
            pltpu.VMEM(lead + (per, width), jnp.float32),
        ] * 2

    coarse, relative = pl.pallas_call(
        functools.partial(coarsen, n, groups, across),
        in_specs=[SMEM, HBM] + [VMEM] * 8,
        out_specs=(VMEM, VMEM),
        out_shape=(
            jax.ShapeDtypeStruct((count // 8, 2, rows, width), jnp.float32),
            jax.ShapeDtypeStruct((owned // 8, width), jnp.float32),
        ),
        scratch_shapes=[
            pltpu.VMEM(match_one.shape, jnp.int32),
            pltpu.VMEM((count, width, width), jnp.bfloat16),
            pltpu.VMEM((ROWS, lanes), jnp.int32),
            pltpu.VMEM((n, ROWS, lanes), jnp.int32),
            pltpu.VMEM((groups, ROWS, lanes), jnp.int32),
            pltpu.VMEM((n, owned, width), jnp.float32),
            pltpu.VMEM((owned, width), jnp.float32),
            pltpu.VMEM((groups, owned, width), jnp.float32),
            pltpu.VMEM((plan_rows, lanes), jnp.int32),
            pltpu.SMEM((plan_rows, lanes), jnp.int32),
            pltpu.VMEM((ROWS, lanes), jnp.int32),
            pltpu.SMEM((ROWS, lanes), jnp.int32),
            pltpu.VMEM((owned // 8, width), jnp.float32),
            pltpu.VMEM((count + 1, width, width), jnp.float32),
            *message(ring, chips, per=2 * per),
            *message(groups, 2, hop_one),
            *message(groups, 2, hop_two),
            *message(2 * groups)[:2],
            *message(groups, 2)[:2],
            pltpu.VMEM((groups * per + 1, 2, rows, width), jnp.float32),
            pltpu.VMEM((per * (rows + 2), width), jnp.int16),
            pltpu.VMEM((2 * per * (rows + 2), width), jnp.int16),
            pltpu.SemaphoreType.DMA((2,)),
            pltpu.SemaphoreType.DMA((2,)),
            pltpu.SemaphoreType.DMA((2,)),
            pltpu.SemaphoreType.DMA((2,)),
            pltpu.SemaphoreType.DMA((ring, 2)),
            pltpu.SemaphoreType.DMA((ring, chips)),
            pltpu.SemaphoreType.DMA((2, 2)),
            pltpu.SemaphoreType.DMA((groups, 2, hop_one)),
            pltpu.SemaphoreType.DMA((2, 2)),
            pltpu.SemaphoreType.DMA((groups, 2, hop_two)),
            pltpu.SemaphoreType.DMA((2,)),
            pltpu.SemaphoreType.DMA((groups, 2)),
            pltpu.SemaphoreType.DMA((count // math.gcd(count, 16),)),
            pltpu.SemaphoreType.DMA((2,)),
            pltpu.SemaphoreType.REGULAR,
        ],
        compiler_params=pltpu.CompilerParams(
            collective_id=0,
            has_side_effects=True,
            vmem_limit_bytes=VMEM_BYTES,
        ),
    )(
        ids_one,
        blocks,
        ids_one,
        target_one[None],
        target_two[None],
        target_three[None],
        vertex_weights,
        match_one,
        match_two,
        match_three,
    )
    pieces = math.gcd(count // 8, 4)
    coarse, relative = pl.pallas_call(
        hand_on,
        in_specs=[HBM, HBM],
        out_specs=(HBM, HBM),
        out_shape=(
            jax.ShapeDtypeStruct(coarse.shape, jnp.float32),
            jax.ShapeDtypeStruct(relative.shape, jnp.float32),
        ),
        scratch_shapes=[
            pltpu.VMEM(coarse.shape, jnp.float32),
            pltpu.VMEM(relative.shape, jnp.float32),
            pltpu.SemaphoreType.DMA((pieces + 1,)),
            pltpu.SemaphoreType.DMA((pieces + 1,)),
        ],
    )(coarse, relative)
    return coarse.reshape(count // 8, width, width), relative


def solution(mesh):
    both = ("grp", "dev")
    return jax.shard_map(
        per_device,
        mesh=mesh,
        in_specs=(
            P(both, None, None),
            P(None, both),
            P(None, both),
            P(None, both),
            P(),
            P(),
            P(),
            P(both),
            P(both),
            P(both),
            P(both, None),
        ),
        out_specs=(P(both, None, None), P(both, None)),
        check_vma=False,
    )
```

```python
import functools
import math

import jax
import jax.numpy as jnp
from jax import lax
from jax.experimental import pallas as pl
from jax.experimental.pallas import tpu as pltpu
from jax.sharding import PartitionSpec as P

LEVELS = 32767.0
TINY = 1e-30
NT = (((1,), (1,)), ((), ()))
ROWS = 8


def hot(row, rows):
    names = lax.broadcasted_iota(jnp.int32, (rows, row.shape[1]), 0)
    return (names == row).astype(jnp.bfloat16)


def halves(x):
    high = x.astype(jnp.bfloat16)
    low = (x - high.astype(jnp.float32)).astype(jnp.bfloat16)
    return high, low


def project(block, row, col):
    left = hot(row, row.shape[1])
    halfway = jnp.dot(left, block, preferred_element_type=jnp.float32)
    right = hot(col, col.shape[1])
    both = jnp.concatenate([right, right], axis=1)
    split = jnp.concatenate(halves(halfway), axis=1)
    return lax.dot_general(split, both, NT, preferred_element_type=jnp.float32)


def encode(parts):
    tops = functools.reduce(jnp.maximum, [jnp.abs(part) for part in parts])
    peak = jnp.maximum(jnp.max(tops, axis=0, keepdims=True), TINY)
    up = LEVELS / peak
    codes = [jnp.round(part * up).astype(jnp.int32).astype(jnp.int16) for part in parts]
    return codes, peak * (1.0 / LEVELS)


def decode(code, scale):
    return code.astype(jnp.int32).astype(jnp.float32) * scale


def lookup(table, index):
    return jnp.take_along_axis(table, index, axis=1, mode="promise_in_bounds")


def fold(weights, row):
    width = row.shape[1]
    place = lax.broadcasted_iota(jnp.int32, (ROWS, width), 0)
    rest = jnp.broadcast_to(weights, (ROWS, width))
    split = jnp.zeros((ROWS, width), jnp.float32)
    for turn in range(3):
        part = rest.astype(jnp.bfloat16).astype(jnp.float32)
        rest = rest - part
        split = jnp.where(place == turn, part, split)
    right = hot(row, width)
    return lax.dot_general(split.astype(jnp.bfloat16), right, NT, preferred_element_type=jnp.float32)


def column(row):
    lanes = row.shape[1]
    return jnp.broadcast_to(row, (lanes, lanes)).T


def latest(match, order):
    return jnp.max(jnp.where(match, order, -1), axis=0, keepdims=True)


def coarsen(
    n,
    groups,
    across,
    blocks,
    *rest,
):
    given, rest = rest[:8], rest[8:]
    (coarse, relative), rest = rest[:2], rest[2:]
    held, rest = rest[:9], rest[9:]
    body(n, groups, across, blocks, given, held, coarse, relative, *rest)


def body(
    n,
    groups,
    across,
    blocks,
    given,
    inputs,
    coarse,
    relative,
    table,
    own,
    labels,
    land_labels,
    land_far,
    land_weight,
    near_weight,
    land_weight_far,
    plan,
    plan_smem,
    plan_third,
    third_smem,
    coarse_weight,
    sums,
    out_half,
    out_scale_half,
    land_half,
    land_scale_half,
    out_one,
    out_scale_one,
    land_one,
    land_scale_one,
    out_two,
    out_scale_two,
    land_two,
    land_scale_two,
    out_three,
    out_scale_three,
    land_three,
    land_scale_three,
    sums_three,
    bulk,
    bulk_half,
    near_send,
    near_recv,
    far_send,
    far_recv,
    half_send,
    half_recv,
    one_send,
    one_recv,
    two_send,
    two_recv,
    three_send,
    three_recv,
    own_sem,
    input_sem,
    local,
    free,
):
    ids_smem, ids, target_one, target_two, target_three, weight, match_one, match_two, match_three = inputs
    me = lax.axis_index("dev")
    group = lax.axis_index("grp")
    core, chip = me % 2, me // 2
    sibling = me + 1 - 2 * core
    chips = n // 2
    down = chips // across
    my_x, my_y = chip % across, chip // across
    count = own.shape[0]
    width = own.shape[2]
    rows = width // 2
    lanes = labels.shape[1]
    per_one, per_two, slots_two = count // n, count // 2 // n, count // 4
    per_three = slots_two // groups
    quarter = match_three.shape[0]
    ring = out_half.shape[0]
    trips = own_sem.shape[0]
    unroll = count // trips
    middle = trips * 3 // 4
    sizes = ((across, down), (down, across))

    def peer(step):
        return lax.rem(me + step, n)

    def source(step):
        return lax.rem(me - step + n, n)

    def far_peer(step):
        return lax.rem(group + step, groups)

    def far_source(step):
        return lax.rem(group - step + groups, groups)

    def remote(src, dst, send, recv, device):
        return pltpu.make_async_remote_copy(
            src_ref=src,
            dst_ref=dst,
            send_sem=send,
            recv_sem=recv,
            device_id=device,
            device_id_type=pl.DeviceIdType.MESH,
        )

    def settle(ref, sem):
        pltpu.make_async_copy(ref, ref, sem).wait()

    def send_labels(v, here):
        return remote(labels, land_labels.at[here], near_send.at[0], near_recv.at[0], {"dev": v})

    def send_weight(v, here):
        return remote(weight, land_weight.at[here], near_send.at[1], near_recv.at[1], {"dev": v})

    def send_labels_far(v, here):
        return remote(labels, land_far.at[here], far_send.at[0], far_recv.at[0], {"grp": v})

    def send_weight_far(v, here):
        return remote(
            near_weight, land_weight_far.at[here], far_send.at[1], far_recv.at[1], {"grp": v}
        )

    def own_copy(i):
        part = pl.ds(i * unroll, unroll)
        return pltpu.make_async_copy(blocks.at[part], own.at[part], own_sem.at[i])

    def send_half(i, dx, dy):
        at, r = i % ring, dy * across + dx
        return (
            remote(
                out_half.at[at, r], land_half.at[at, r], half_send.at[at, 0], half_recv.at[at, r],
                {"dev": sibling},
            ),
            remote(
                out_scale_half.at[at, r], land_scale_half.at[at, r], half_send.at[at, 1],
                half_recv.at[at, r], {"dev": sibling},
            ),
        )

    def chip_at(b, first, second):
        return second * across + first if b == 0 else first * across + second

    def here_of(b):
        return (my_x, my_y) if b == 0 else (my_y, my_x)

    def send_one(i, b, step, turn):
        z, w = sizes[b]
        first, second = here_of(b)
        m = (step - 1) * w + turn
        to = chip_at(b, (first + step) % z, second) * 2 + core
        return (
            remote(
                out_one.at[i, b, m], land_one.at[i, b, m], one_send.at[b, 0],
                one_recv.at[i, b, m], {"dev": to},
            ),
            remote(
                out_scale_one.at[i, b, m], land_scale_one.at[i, b, m], one_send.at[b, 1],
                one_recv.at[i, b, m], {"dev": to},
            ),
        )

    def send_two(i, b, turn):
        w = sizes[b][1]
        first, second = here_of(b)
        m = turn - 1
        to = chip_at(b, first, (second + turn) % w) * 2 + core
        return (
            remote(
                out_two.at[i, b, m], land_two.at[i, b, m], two_send.at[b, 0],
                two_recv.at[i, b, m], {"dev": to},
            ),
            remote(
                out_scale_two.at[i, b, m], land_scale_two.at[i, b, m], two_send.at[b, 1],
                two_recv.at[i, b, m], {"dev": to},
            ),
        )

    def send_three(i, b, to_group, from_group, from_core):
        device = {"grp": to_group, "dev": chip * 2 + b}
        return (
            remote(
                out_three.at[i * 2 + b], land_three.at[from_group, from_core], three_send.at[0],
                three_recv.at[from_group, from_core], device,
            ),
            remote(
                out_scale_three.at[i * 2 + b], land_scale_three.at[from_group, from_core],
                three_send.at[1], three_recv.at[from_group, from_core], device,
            ),
        )

    def chunk_group(i):
        falling = groups - 1 - i
        low = jnp.where(falling > group, falling, falling - 1)
        high = jnp.where(i < group, i, i + 1)
        other = jnp.where(group < groups // 2, low, high)
        return jnp.where(i == groups - 1, group, other)

    barrier = pltpu.get_barrier_semaphore()

    @pl.loop(1, n)
    def _(step):
        pl.semaphore_signal(
            barrier, inc=1, device_id={"dev": peer(step)}, device_id_type=pl.DeviceIdType.MESH
        )

    @pl.loop(1, groups)
    def _(step):
        v = far_peer(step)
        pl.semaphore_signal(
            barrier, inc=1, device_id={"grp": v}, device_id_type=pl.DeviceIdType.MESH
        )
        pl.semaphore_signal(
            barrier, inc=1, device_id={"grp": v, "dev": sibling}, device_id_type=pl.DeviceIdType.MESH
        )

    sources = (given[0], *given)
    loads = [pltpu.make_async_copy(a, v, input_sem.at[i]) for i, (a, v) in enumerate(zip(sources, inputs))]
    for load in loads[1:5] + loads[:1] + loads[5:]:
        load.start()
    for i in range(trips):
        own_copy(i).start()
    for load in loads:
        load.wait()
    labels[...] = jnp.zeros(labels.shape, jnp.int32)
    labels[0:2, 0:count] = ids[...]
    labels[2:3, 0:count] = target_one[...]
    labels[3:4, 0 : count // 2] = target_two[...]
    labels[4:5, 0 : count // 4] = target_three[...]
    named = labels[...]
    land_labels[me] = named
    land_far[group] = named

    pl.semaphore_wait(barrier, n - 1 + 2 * (groups - 1))

    @pl.loop(1, n)
    def _(step):
        send_labels(peer(step), me).start()
        send_weight(peer(step), me).start()

    @pl.loop(1, groups)
    def _(step):
        send_labels_far(far_peer(step), group).start()

    for turn in range(4):
        one = match_one[pl.ds(turn, quarter, stride=4), :]
        two = match_two[pl.ds(turn // 2, quarter, stride=2), :]
        table[turn * quarter : (turn + 1) * quarter, :] = lookup(match_three[...], lookup(two, one))

    def mapping(b):
        return table[pl.ds((b % 4) * quarter + b // 4, 1), :]

    none = count
    sums[none] = jnp.zeros(sums.shape[1:], jnp.float32)
    sums_three[groups * per_three] = jnp.zeros(sums_three.shape[1:], jnp.float32)

    def level(i, chained):
        own_copy(i).wait()
        parts = []
        for j in range(unroll):
            k = i * unroll + j
            row, col = mapping(ids_smem[0, k]), mapping(ids_smem[1, k])
            parts.append(project(own[k], row, col))
        for j in range(unroll):
            k = i * unroll + j
            sums[k] = parts[j] + sums[plan_smem[0, k] if chained else none]

    @pl.loop(0, max(middle - 1, 0))
    def _(i):
        level(i, False)

    settle(land_labels.at[pl.ds(0, n - 1)], near_recv.at[0])

    square = (lanes, lanes)
    lane = lax.broadcasted_iota(jnp.int32, (1, lanes), 1)
    order_down = lax.broadcasted_iota(jnp.int32, square, 0)
    order_across = lax.broadcasted_iota(jnp.int32, square, 1)

    def slots_of(mine):
        first = mine[2:3, :]
        spread = jnp.broadcast_to(first, mine.shape)
        second = jnp.zeros((1, lanes), jnp.int32)
        for o in range(n):
            second = jnp.where(lane // per_one == o, lookup(land_labels[o], spread)[3:4, :], second)
        return first // per_two * slots_two + second

    slot_own = slots_of(named)
    down_own = column(slot_own)
    before = latest((down_own == slot_own) & (order_down < order_across), order_down)
    plan[0:1, :] = jnp.where(before < 0, none, before)
    blocks_of_slots = -(-n * slots_two // lanes)
    for part in range(blocks_of_slots):
        name = order_across + part * lanes
        last = latest(down_own == name, order_down)
        plan[1 + part : 2 + part, :] = jnp.where(last < 0, none, last)
    rest = plan.shape[0] - 1 - blocks_of_slots
    if rest:
        plan[1 + blocks_of_slots :, :] = jnp.zeros((rest, lanes), jnp.int32)
    to_smem = pltpu.make_async_copy(plan, plan_smem, local.at[1])
    to_smem.start()

    @pl.loop(max(middle - 1, 0), middle)
    def _(i):
        level(i, False)

    to_smem.wait()

    @pl.loop(0, middle)
    def _(i):
        for j in range(unroll):
            k = i * unroll + j
            sums[k] = sums[k] + sums[plan_smem[0, k]]

    @pl.loop(middle, trips)
    def _(i):
        level(i, True)

    def from_own(to_chip, b, i, j, h):
        slot = (to_chip * 2 + b) * slots_two + chunk_group(i) * per_three + j
        spot = plan_smem[1 + slot // lanes, slot % lanes]
        return sums[spot, pl.ds(pl.multiple_of(h * rows, rows), rows), :]

    def held_here(b, i, dx, dy):
        to = (my_y + dy) % down * across + (my_x + dx) % across
        at, r = i % ring, dy * across + dx
        parts = []
        for j in range(per_three):
            m = b * per_three + j
            part = decode(land_half[at, r, m], land_scale_half[at, r])
            parts.append(part + from_own(to, b, i, j, core))
        return parts

    places = [(dx, dy) for dy in range(down) for dx in range(across)]
    places.sort(key=lambda p: (p[0] == 0) + (p[1] == 0))

    def spread(i):
        if ring < groups:

            @pl.when(i >= ring)
            def _():
                pl.semaphore_wait(free, 1)
                settle(out_half.at[i % ring], half_send.at[i % ring, 0])
                settle(out_scale_half.at[i % ring], half_send.at[i % ring, 1])

        for dx, dy in places:
            to = (my_y + dy) % down * across + (my_x + dx) % across
            at, r = i % ring, dy * across + dx
            parts = [from_own(to, b, i, j, 1 - core) for b in range(2) for j in range(per_three)]
            pack(parts, out_half.at[at, r], out_scale_half.at[at, r])
            start(send_half(i, dx, dy))

    def release(i):
        if ring < groups:

            @pl.when(i < groups - ring)
            def _():
                pl.semaphore_signal(
                    free, inc=1, device_id={"dev": sibling}, device_id_type=pl.DeviceIdType.MESH
                )

    def pack(parts, codes, scales):
        packed, scales[...] = encode(parts)
        for j, code in enumerate(packed):
            codes[j] = code

    def start(copies):
        for copy in copies:
            copy.start()

    def offset(b, first, second):
        return (first, second) if b == 0 else (second, first)

    def turns(b):
        w = sizes[b][1]
        return [*range(1, w), 0]

    def first_hop(i):
        here = set()
        for spot in range(max(across, down)):
            for b in range(2):
                z, w = sizes[b]
                if spot >= w:
                    continue
                turn = turns(b)[spot]
                for step in range(1, z):
                    m = (step - 1) * w + turn
                    place = offset(b, step, turn)
                    if place not in here:
                        here.add(place)
                        settle(bulk_half, half_recv.at[i % ring, place[1] * across + place[0]])
                    parts = held_here(b, i, *place)
                    pack(parts, out_one.at[i, b, m], out_scale_one.at[i, b, m])
                    start(send_one(i, b, step, turn))

    def with_first(parts, i, b, turn):
        z, w = sizes[b]
        for step in range(1, z):
            m = (step - 1) * w + turn
            settle(bulk, one_recv.at[i, b, m])
            parts = [
                p + decode(land_one[i, b, m, j], land_scale_one[i, b, m])
                for j, p in enumerate(parts)
            ]
        return parts

    def second_hop(i):
        for b in range(2):
            w = sizes[b][1]
            for turn in range(1, w):
                parts = held_here(b, i, *offset(b, 0, turn))
                parts = with_first(parts, i, b, turn)
                pack(parts, out_two.at[i, b, turn - 1], out_scale_two.at[i, b, turn - 1])
                start(send_two(i, b, turn))

    def reduced(i):
        settle(bulk_half, half_recv.at[i % ring, 0])
        for b in range(2):
            w = sizes[b][1]
            parts = held_here(b, i, 0, 0)
            parts = with_first(parts, i, b, 0)
            for turn in range(1, w):
                settle(bulk, two_recv.at[i, b, turn - 1])
                parts = [
                    p + decode(land_two[i, b, turn - 1, j], land_scale_two[i, b, turn - 1])
                    for j, p in enumerate(parts)
                ]
            pack(parts, out_three.at[i * 2 + b], out_scale_three.at[i * 2 + b])
        release(i)

    def third_hop(i):
        reduced(i)
        for b in range(2):
            start(send_three(i, b, chunk_group(i), group, core))

    spread(0)

    settle(land_far.at[pl.ds(0, groups - 1)], far_recv.at[0])

    total = groups * per_three
    pick = jnp.broadcast_to(group * per_three + lane % per_three, (ROWS, lanes))
    third = jnp.full((1, lanes), -1, jnp.int32)
    for u in range(groups):
        third = jnp.where(lane // per_three == u, lookup(land_far[u], pick)[4:5, :], third)
    down_third = column(third)

    def rank(k):
        return (group - k // per_three - 1 + groups) % groups * per_three + k % per_three

    rank_down, rank_across = rank(order_down), rank(order_across)
    real = order_down < total
    before = latest(real & (down_third == third) & (rank_down < rank_across), rank_down)
    last = latest(real & (down_third == order_across), rank_down)
    plan_third[0:1, :] = jnp.where(before < 0, total, before)
    plan_third[1:2, :] = jnp.where(last < 0, total, last)
    plan_third[2:, :] = jnp.zeros((plan_third.shape[0] - 2, lanes), jnp.int32)
    third_to_smem = pltpu.make_async_copy(plan_third, third_smem, local.at[0])
    third_to_smem.start()

    settle(land_weight.at[pl.ds(0, n - 1)], near_recv.at[1])

    held = weight[...]
    for step in range(1, n):
        held = held + land_weight[peer(step)]
    near_weight[...] = held

    @pl.loop(1, groups)
    def _(step):
        send_weight_far(far_peer(step), group).start()

    @pl.loop(0, groups)
    def _(i):
        first_hop(i)

        @pl.when(i > 0)
        def _():
            third_hop(i - 1)

        @pl.when(i + 1 < groups)
        def _():
            spread(i + 1)

        second_hop(i)

    owned = weight.shape[0]
    start_row = (group * n + me) * (owned // 4)
    for e in range(owned // 8):
        folded = jnp.zeros((ROWS, width), jnp.float32)
        for f in range(8 * e, 8 * e + 8):
            row = table[pl.ds(f % 4 * quarter + start_row + f // 4, 1), :]
            folded = folded + fold(weight[f : f + 1, :], row)
        coarse_weight[e : e + 1, :] = jnp.sum(folded, axis=0, keepdims=True)
    held = near_weight[...]
    settle(land_weight_far.at[pl.ds(0, groups - 1)], far_recv.at[1])
    for step in range(1, groups):
        held = held + land_weight_far[far_source(step)]
    whole = jnp.sum(jnp.sum(held, axis=0, keepdims=True), axis=1, keepdims=True)
    vertices = relative.shape[0] * n * groups * relative.shape[1]
    relative[...] = coarse_weight[...] * vertices / whole

    third_to_smem.wait()
    end = groups - 1

    def take(codes, scales, at, h, u):
        for j in range(per_three):
            part = decode(codes[j], scales[...])
            sums_three[at + j, h] = part + sums_three[third_smem[0, u * per_three + j], h]

    @pl.loop(1, groups)
    def _(step):
        u = far_source(step)
        for h in range(2):
            settle(bulk, three_recv.at[u, h])
            take(land_three.at[u, h], land_scale_three.at[u, h], (step - 1) * per_three, h, u)

    reduced(end)
    start(send_three(end, 1 - core, group, group, core))

    take(out_three.at[end * 2 + core], out_scale_three.at[end * 2 + core], end * per_three, core, group)
    other = 1 - core
    settle(bulk, three_recv.at[group, other])
    take(land_three.at[group, other], land_scale_three.at[group, other], end * per_three, other, group)

    @pl.loop(0, coarse.shape[0])
    def _(slot):
        coarse[slot] = sums_three[third_smem[1, slot]]

    settle(land_labels.at[pl.ds(0, n - 1)], near_send.at[0])
    settle(land_weight.at[pl.ds(0, n - 1)], near_send.at[1])
    settle(land_far.at[pl.ds(0, groups - 1)], far_send.at[0])
    settle(land_weight_far.at[pl.ds(0, groups - 1)], far_send.at[1])
    for at in range(ring):
        settle(out_half.at[at], half_send.at[at, 0])
        settle(out_scale_half.at[at], half_send.at[at, 1])
    for b in range(2):
        z, w = sizes[b]
        some, few = pl.ds(0, (z - 1) * w), pl.ds(0, w - 1)
        settle(out_one.at[pl.ds(0, groups), b, some], one_send.at[b, 0])
        settle(out_scale_one.at[pl.ds(0, groups), b, some], one_send.at[b, 1])
        settle(out_two.at[pl.ds(0, groups), b, few], two_send.at[b, 0])
        settle(out_scale_two.at[pl.ds(0, groups), b, few], two_send.at[b, 1])
    settle(out_three.at[pl.ds(0, 2 * groups - 1)], three_send.at[0])
    settle(out_scale_three.at[pl.ds(0, 2 * groups - 1)], three_send.at[1])


def hand_on(coarse_in, relative_in, coarse, relative, blocks, row, arrive, leave):
    pieces = arrive.shape[0] - 1
    size = blocks.shape[0] // pieces
    moves = [(coarse_in, blocks, coarse, pl.ds(i * size, size)) for i in range(pieces)]
    moves.append((relative_in, row, relative, pl.ds(0, row.shape[0])))
    ins = [pltpu.make_async_copy(a.at[p], v.at[p], arrive.at[i]) for i, (a, v, _, p) in enumerate(moves)]
    outs = [pltpu.make_async_copy(v.at[p], b.at[p], leave.at[i]) for i, (_, v, b, p) in enumerate(moves)]
    for copy in ins:
        copy.start()
    for first, second in zip(ins, outs):
        first.wait()
        second.start()
    for copy in outs:
        copy.wait()


VMEM = pl.BlockSpec(memory_space=pltpu.VMEM)
HBM = pl.BlockSpec(memory_space=pl.ANY)
VMEM_BYTES = 67_043_328


def per_device(
    blocks,
    ids_one,
    ids_two,
    ids_three,
    match_one,
    match_two,
    match_three,
    target_one,
    target_two,
    target_three,
    vertex_weights,
):
    n, groups = lax.axis_size("dev"), lax.axis_size("grp")
    count, width = blocks.shape[0], blocks.shape[1]
    rows = width // 2
    lanes = -(-count // width) * width
    owned = vertex_weights.shape[0]
    slots = count // 4
    per = slots // groups
    chips = n // 2
    across = 1
    while across * across < chips:
        across *= 2
    down = chips // across
    hop_one = max((across - 1) * down, (down - 1) * across, 1)
    hop_two = max(across - 1, down - 1, 1)
    plan_rows = -(-(1 + -(-n * slots // lanes)) // ROWS) * ROWS
    half_bytes = groups * chips * 4 * per * rows * width * 2
    ring = groups if half_bytes <= VMEM_BYTES // 4 else 2

    def message(*lead, per=per):
        return [
            pltpu.VMEM(lead + (per, rows, width), jnp.int16),
            pltpu.VMEM(lead + (1, width), jnp.float32),
        ] * 2

    targets = [x[None] for x in (target_one, target_two, target_three)]
    small = [ids_one, *targets, vertex_weights, match_one, match_two, match_three]
    coarse, relative = pl.pallas_call(
        functools.partial(coarsen, n, groups, across),
        in_specs=[HBM] * 9,
        out_specs=(VMEM, VMEM),
        out_shape=(
            jax.ShapeDtypeStruct((count // 8, 2, rows, width), jnp.float32),
            jax.ShapeDtypeStruct((owned // 8, width), jnp.float32),
        ),
        scratch_shapes=[
            pltpu.SMEM(ids_one.shape, jnp.int32),
            *[pltpu.VMEM(x.shape, x.dtype) for x in small],
            pltpu.VMEM(match_one.shape, jnp.int32),
            pltpu.VMEM((count, width, width), jnp.bfloat16),
            pltpu.VMEM((ROWS, lanes), jnp.int32),
            pltpu.VMEM((n, ROWS, lanes), jnp.int32),
            pltpu.VMEM((groups, ROWS, lanes), jnp.int32),
            pltpu.VMEM((n, owned, width), jnp.float32),
            pltpu.VMEM((owned, width), jnp.float32),
            pltpu.VMEM((groups, owned, width), jnp.float32),
            pltpu.VMEM((plan_rows, lanes), jnp.int32),
            pltpu.SMEM((plan_rows, lanes), jnp.int32),
            pltpu.VMEM((ROWS, lanes), jnp.int32),
            pltpu.SMEM((ROWS, lanes), jnp.int32),
            pltpu.VMEM((owned // 8, width), jnp.float32),
            pltpu.VMEM((count + 1, width, width), jnp.float32),
            *message(ring, chips, per=2 * per),
            *message(groups, 2, hop_one),
            *message(groups, 2, hop_two),
            *message(2 * groups)[:2],
            *message(groups, 2)[:2],
            pltpu.VMEM((groups * per + 1, 2, rows, width), jnp.float32),
            pltpu.VMEM((per * rows // 2 + 1, 1, width), jnp.float32),
            pltpu.VMEM((per * rows + 1, 1, width), jnp.float32),
            pltpu.SemaphoreType.DMA((2,)),
            pltpu.SemaphoreType.DMA((2,)),
            pltpu.SemaphoreType.DMA((2,)),
            pltpu.SemaphoreType.DMA((2,)),
            pltpu.SemaphoreType.DMA((ring, 2)),
            pltpu.SemaphoreType.DMA((ring, chips)),
            pltpu.SemaphoreType.DMA((2, 2)),
            pltpu.SemaphoreType.DMA((groups, 2, hop_one)),
            pltpu.SemaphoreType.DMA((2, 2)),
            pltpu.SemaphoreType.DMA((groups, 2, hop_two)),
            pltpu.SemaphoreType.DMA((2,)),
            pltpu.SemaphoreType.DMA((groups, 2)),
            pltpu.SemaphoreType.DMA((count // math.gcd(count, 16),)),
            pltpu.SemaphoreType.DMA((9,)),
            pltpu.SemaphoreType.DMA((2,)),
            pltpu.SemaphoreType.REGULAR,
        ],
        compiler_params=pltpu.CompilerParams(
            collective_id=0,
            has_side_effects=True,
            vmem_limit_bytes=VMEM_BYTES,
        ),
    )(
        blocks,
        *small,
    )
    pieces = math.gcd(count // 8, 4)
    coarse, relative = pl.pallas_call(
        hand_on,
        in_specs=[HBM, HBM],
        out_specs=(HBM, HBM),
        out_shape=(
            jax.ShapeDtypeStruct(coarse.shape, jnp.float32),
            jax.ShapeDtypeStruct(relative.shape, jnp.float32),
        ),
        scratch_shapes=[
            pltpu.VMEM(coarse.shape, jnp.float32),
            pltpu.VMEM(relative.shape, jnp.float32),
            pltpu.SemaphoreType.DMA((pieces + 1,)),
            pltpu.SemaphoreType.DMA((pieces + 1,)),
        ],
    )(coarse, relative)
    return coarse.reshape(count // 8, width, width), relative


def solution(mesh):
    both = ("grp", "dev")
    return jax.shard_map(
        per_device,
        mesh=mesh,
        in_specs=(
            P(both, None, None),
            P(None, both),
            P(None, both),
            P(None, both),
            P(),
            P(),
            P(),
            P(both),
            P(both),
            P(both),
            P(both, None),
        ),
        out_specs=(P(both, None, None), P(both, None)),
        check_vma=False,
    )
```

```python
import functools
import math

import jax
import jax.numpy as jnp
from jax import lax
from jax.experimental import pallas as pl
from jax.experimental.pallas import tpu as pltpu
from jax.sharding import PartitionSpec as P

LEVELS = 32767.0
TINY = 1e-30
NT = (((1,), (1,)), ((), ()))
ROWS = 8


def hot(row, rows):
    names = lax.broadcasted_iota(jnp.int32, (rows, row.shape[1]), 0)
    return (names == row).astype(jnp.bfloat16)


def halves(x):
    high = x.astype(jnp.bfloat16)
    low = (x - high.astype(jnp.float32)).astype(jnp.bfloat16)
    return high, low


def project(block, row, col):
    left = hot(row, row.shape[1])
    halfway = jnp.dot(left, block, preferred_element_type=jnp.float32)
    right = hot(col, col.shape[1])
    both = jnp.concatenate([right, right], axis=1)
    split = jnp.concatenate(halves(halfway), axis=1)
    return lax.dot_general(split, both, NT, preferred_element_type=jnp.float32)


def encode(parts):
    tops = functools.reduce(jnp.maximum, [jnp.abs(part) for part in parts])
    peak = jnp.maximum(jnp.max(tops, axis=0, keepdims=True), TINY)
    up = LEVELS / peak
    codes = [jnp.round(part * up).astype(jnp.int32).astype(jnp.int16) for part in parts]
    return codes, peak * (1.0 / LEVELS)


def decode(code, scale):
    return code.astype(jnp.int32).astype(jnp.float32) * scale


def lookup(table, index):
    return jnp.take_along_axis(table, index, axis=1, mode="promise_in_bounds")


def fold(weights, row):
    width = row.shape[1]
    place = lax.broadcasted_iota(jnp.int32, (ROWS, width), 0)
    rest = jnp.broadcast_to(weights, (ROWS, width))
    split = jnp.zeros((ROWS, width), jnp.float32)
    for turn in range(3):
        part = rest.astype(jnp.bfloat16).astype(jnp.float32)
        rest = rest - part
        split = jnp.where(place == turn, part, split)
    right = hot(row, width)
    return lax.dot_general(split.astype(jnp.bfloat16), right, NT, preferred_element_type=jnp.float32)


def column(row):
    lanes = row.shape[1]
    return jnp.broadcast_to(row, (lanes, lanes)).T


def latest(match, order):
    return jnp.max(jnp.where(match, order, -1), axis=0, keepdims=True)


def coarsen(
    n,
    groups,
    across,
    blocks,
    *rest,
):
    given, rest = rest[:8], rest[8:]
    (coarse, relative), rest = rest[:2], rest[2:]
    held, rest = rest[:9], rest[9:]
    body(n, groups, across, blocks, given, held, coarse, relative, *rest)


def body(
    n,
    groups,
    across,
    blocks,
    given,
    inputs,
    coarse,
    relative,
    table,
    own,
    labels,
    land_labels,
    land_far,
    land_weight,
    near_weight,
    land_weight_far,
    plan,
    plan_smem,
    plan_third,
    third_smem,
    coarse_weight,
    sums,
    out_half,
    out_scale_half,
    land_half,
    land_scale_half,
    out_one,
    out_scale_one,
    land_one,
    land_scale_one,
    out_two,
    out_scale_two,
    land_two,
    land_scale_two,
    out_three,
    out_scale_three,
    land_three,
    land_scale_three,
    sums_three,
    bulk,
    bulk_half,
    near_send,
    near_recv,
    far_send,
    far_recv,
    half_send,
    half_recv,
    one_send,
    one_recv,
    two_send,
    two_recv,
    three_send,
    three_recv,
    own_sem,
    input_sem,
    local,
    free,
):
    ids_smem, ids, target_one, target_two, target_three, weight, match_one, match_two, match_three = inputs
    me = lax.axis_index("dev")
    group = lax.axis_index("grp")
    core, chip = me % 2, me // 2
    sibling = me + 1 - 2 * core
    chips = n // 2
    down = chips // across
    my_x, my_y = chip % across, chip // across
    count = own.shape[0]
    width = own.shape[2]
    rows = width // 2
    lanes = labels.shape[1]
    per_one, per_two, slots_two = count // n, count // 2 // n, count // 4
    per_three = slots_two // groups
    quarter = match_three.shape[0]
    ring = out_half.shape[0]
    trips = own_sem.shape[0]
    unroll = count // trips
    middle = trips * 3 // 4
    sizes = ((across, down), (down, across))

    def peer(step):
        return lax.rem(me + step, n)

    def source(step):
        return lax.rem(me - step + n, n)

    def far_peer(step):
        return lax.rem(group + step, groups)

    def far_source(step):
        return lax.rem(group - step + groups, groups)

    def remote(src, dst, send, recv, device):
        return pltpu.make_async_remote_copy(
            src_ref=src,
            dst_ref=dst,
            send_sem=send,
            recv_sem=recv,
            device_id=device,
            device_id_type=pl.DeviceIdType.MESH,
        )

    def settle(ref, sem):
        pltpu.make_async_copy(ref, ref, sem).wait()

    def send_labels(v, here):
        return remote(labels, land_labels.at[here], near_send.at[0], near_recv.at[0], {"dev": v})

    def send_weight(v, here):
        return remote(weight, land_weight.at[here], near_send.at[1], near_recv.at[1], {"dev": v})

    def send_labels_far(v, here):
        return remote(labels, land_far.at[here], far_send.at[0], far_recv.at[0], {"grp": v})

    def send_weight_far(v, here):
        return remote(
            near_weight, land_weight_far.at[here], far_send.at[1], far_recv.at[1], {"grp": v}
        )

    def own_copy(i):
        part = pl.ds(i * unroll, unroll)
        return pltpu.make_async_copy(blocks.at[part], own.at[part], own_sem.at[i])

    def send_half(i, dx, dy):
        at, r = i % ring, dy * across + dx
        return (
            remote(
                out_half.at[at, r], land_half.at[at, r], half_send.at[at, 0], half_recv.at[at, r],
                {"dev": sibling},
            ),
            remote(
                out_scale_half.at[at, r], land_scale_half.at[at, r], half_send.at[at, 1],
                half_recv.at[at, r], {"dev": sibling},
            ),
        )

    def chip_at(b, first, second):
        return second * across + first if b == 0 else first * across + second

    def here_of(b):
        return (my_x, my_y) if b == 0 else (my_y, my_x)

    def send_one(i, b, step, turn):
        z, w = sizes[b]
        first, second = here_of(b)
        m = (step - 1) * w + turn
        to = chip_at(b, (first + step) % z, second) * 2 + core
        return (
            remote(
                out_one.at[i, b, m], land_one.at[i, b, m], one_send.at[b, 0],
                one_recv.at[i, b, m], {"dev": to},
            ),
            remote(
                out_scale_one.at[i, b, m], land_scale_one.at[i, b, m], one_send.at[b, 1],
                one_recv.at[i, b, m], {"dev": to},
            ),
        )

    def send_two(i, b, turn):
        w = sizes[b][1]
        first, second = here_of(b)
        m = turn - 1
        to = chip_at(b, first, (second + turn) % w) * 2 + core
        return (
            remote(
                out_two.at[i, b, m], land_two.at[i, b, m], two_send.at[b, 0],
                two_recv.at[i, b, m], {"dev": to},
            ),
            remote(
                out_scale_two.at[i, b, m], land_scale_two.at[i, b, m], two_send.at[b, 1],
                two_recv.at[i, b, m], {"dev": to},
            ),
        )

    def send_three(i, b, to_group, from_group, from_core):
        device = {"grp": to_group, "dev": chip * 2 + b}
        return (
            remote(
                out_three.at[i * 2 + b], land_three.at[from_group, from_core], three_send.at[0],
                three_recv.at[from_group, from_core], device,
            ),
            remote(
                out_scale_three.at[i * 2 + b], land_scale_three.at[from_group, from_core],
                three_send.at[1], three_recv.at[from_group, from_core], device,
            ),
        )

    def chunk_group(i):
        falling = groups - 1 - i
        low = jnp.where(falling > group, falling, falling - 1)
        high = jnp.where(i < group, i, i + 1)
        other = jnp.where(group < groups // 2, low, high)
        return jnp.where(i == groups - 1, group, other)

    barrier = pltpu.get_barrier_semaphore()

    @pl.loop(1, n)
    def _(step):
        pl.semaphore_signal(
            barrier, inc=1, device_id={"dev": peer(step)}, device_id_type=pl.DeviceIdType.MESH
        )

    @pl.loop(1, groups)
    def _(step):
        v = far_peer(step)
        pl.semaphore_signal(
            barrier, inc=1, device_id={"grp": v}, device_id_type=pl.DeviceIdType.MESH
        )
        pl.semaphore_signal(
            barrier, inc=1, device_id={"grp": v, "dev": sibling}, device_id_type=pl.DeviceIdType.MESH
        )

    sources = (given[0], *given)
    loads = [pltpu.make_async_copy(a, v, input_sem.at[i]) for i, (a, v) in enumerate(zip(sources, inputs))]
    for load in loads[1:5] + loads[:1] + loads[5:]:
        load.start()
    own_copy(0).start()
    for load in loads:
        load.wait()
    for i in range(1, trips):
        own_copy(i).start()
    labels[...] = jnp.zeros(labels.shape, jnp.int32)
    labels[0:2, 0:count] = ids[...]
    labels[2:3, 0:count] = target_one[...]
    labels[3:4, 0 : count // 2] = target_two[...]
    labels[4:5, 0 : count // 4] = target_three[...]
    named = labels[...]
    land_labels[me] = named
    land_far[group] = named

    for turn in range(4):
        one = match_one[pl.ds(turn, quarter, stride=4), :]
        two = match_two[pl.ds(turn // 2, quarter, stride=2), :]
        table[turn * quarter : (turn + 1) * quarter, :] = lookup(match_three[...], lookup(two, one))

    def mapping(b):
        return table[pl.ds((b % 4) * quarter + b // 4, 1), :]

    none = count
    sums[none] = jnp.zeros(sums.shape[1:], jnp.float32)
    sums_three[groups * per_three] = jnp.zeros(sums_three.shape[1:], jnp.float32)

    def level(i, chained):
        own_copy(i).wait()
        parts = []
        for j in range(unroll):
            k = i * unroll + j
            row, col = mapping(ids_smem[0, k]), mapping(ids_smem[1, k])
            parts.append(project(own[k], row, col))
        for j in range(unroll):
            k = i * unroll + j
            sums[k] = parts[j] + sums[plan_smem[0, k] if chained else none]

    early = min(2, middle)

    @pl.loop(0, early)
    def _(i):
        level(i, False)

    pl.semaphore_wait(barrier, n - 1 + 2 * (groups - 1))

    @pl.loop(1, n)
    def _(step):
        send_labels(peer(step), me).start()
        send_weight(peer(step), me).start()

    @pl.loop(1, groups)
    def _(step):
        send_labels_far(far_peer(step), group).start()

    @pl.loop(early, max(middle - 1, early))
    def _(i):
        level(i, False)

    settle(land_labels.at[pl.ds(0, n - 1)], near_recv.at[0])

    square = (lanes, lanes)
    lane = lax.broadcasted_iota(jnp.int32, (1, lanes), 1)
    order_down = lax.broadcasted_iota(jnp.int32, square, 0)
    order_across = lax.broadcasted_iota(jnp.int32, square, 1)

    def slots_of(mine):
        first = mine[2:3, :]
        spread = jnp.broadcast_to(first, mine.shape)
        second = jnp.zeros((1, lanes), jnp.int32)
        for o in range(n):
            second = jnp.where(lane // per_one == o, lookup(land_labels[o], spread)[3:4, :], second)
        return first // per_two * slots_two + second

    slot_own = slots_of(named)
    down_own = column(slot_own)
    before = latest((down_own == slot_own) & (order_down < order_across), order_down)
    plan[0:1, :] = jnp.where(before < 0, none, before)
    blocks_of_slots = -(-n * slots_two // lanes)
    for part in range(blocks_of_slots):
        name = order_across + part * lanes
        last = latest(down_own == name, order_down)
        plan[1 + part : 2 + part, :] = jnp.where(last < 0, none, last)
    rest = plan.shape[0] - 1 - blocks_of_slots
    if rest:
        plan[1 + blocks_of_slots :, :] = jnp.zeros((rest, lanes), jnp.int32)
    to_smem = pltpu.make_async_copy(plan, plan_smem, local.at[1])
    to_smem.start()

    @pl.loop(max(middle - 1, early), middle)
    def _(i):
        level(i, False)

    to_smem.wait()

    @pl.loop(0, middle)
    def _(i):
        for j in range(unroll):
            k = i * unroll + j
            sums[k] = sums[k] + sums[plan_smem[0, k]]

    @pl.loop(middle, trips)
    def _(i):
        level(i, True)

    def from_own(to_chip, b, i, j, h):
        slot = (to_chip * 2 + b) * slots_two + chunk_group(i) * per_three + j
        spot = plan_smem[1 + slot // lanes, slot % lanes]
        return sums[spot, pl.ds(pl.multiple_of(h * rows, rows), rows), :]

    def held_here(b, i, dx, dy):
        to = (my_y + dy) % down * across + (my_x + dx) % across
        at, r = i % ring, dy * across + dx
        parts = []
        for j in range(per_three):
            m = b * per_three + j
            part = decode(land_half[at, r, m], land_scale_half[at, r])
            parts.append(part + from_own(to, b, i, j, core))
        return parts

    places = [(dx, dy) for dy in range(down) for dx in range(across)]
    places.sort(key=lambda p: (p[0] == 0) + (p[1] == 0))

    def spread(i):
        if ring < groups:

            @pl.when(i >= ring)
            def _():
                pl.semaphore_wait(free, 1)
                settle(out_half.at[i % ring], half_send.at[i % ring, 0])
                settle(out_scale_half.at[i % ring], half_send.at[i % ring, 1])

        for dx, dy in places:
            to = (my_y + dy) % down * across + (my_x + dx) % across
            at, r = i % ring, dy * across + dx
            parts = [from_own(to, b, i, j, 1 - core) for b in range(2) for j in range(per_three)]
            pack(parts, out_half.at[at, r], out_scale_half.at[at, r])
            start(send_half(i, dx, dy))

    def release(i):
        if ring < groups:

            @pl.when(i < groups - ring)
            def _():
                pl.semaphore_signal(
                    free, inc=1, device_id={"dev": sibling}, device_id_type=pl.DeviceIdType.MESH
                )

    def pack(parts, codes, scales):
        packed, scales[...] = encode(parts)
        for j, code in enumerate(packed):
            codes[j] = code

    def start(copies):
        for copy in copies:
            copy.start()

    def offset(b, first, second):
        return (first, second) if b == 0 else (second, first)

    def turns(b):
        w = sizes[b][1]
        return [*range(1, w), 0]

    def first_hop(i):
        here = set()
        for spot in range(max(across, down)):
            for b in range(2):
                z, w = sizes[b]
                if spot >= w:
                    continue
                turn = turns(b)[spot]
                for step in range(1, z):
                    m = (step - 1) * w + turn
                    place = offset(b, step, turn)
                    if place not in here:
                        here.add(place)
                        settle(bulk_half, half_recv.at[i % ring, place[1] * across + place[0]])
                    parts = held_here(b, i, *place)
                    pack(parts, out_one.at[i, b, m], out_scale_one.at[i, b, m])
                    start(send_one(i, b, step, turn))

    def with_first(parts, i, b, turn):
        z, w = sizes[b]
        for step in range(1, z):
            m = (step - 1) * w + turn
            settle(bulk, one_recv.at[i, b, m])
            parts = [
                p + decode(land_one[i, b, m, j], land_scale_one[i, b, m])
                for j, p in enumerate(parts)
            ]
        return parts

    def second_hop(i):
        for b in range(2):
            w = sizes[b][1]
            for turn in range(1, w):
                parts = held_here(b, i, *offset(b, 0, turn))
                parts = with_first(parts, i, b, turn)
                pack(parts, out_two.at[i, b, turn - 1], out_scale_two.at[i, b, turn - 1])
                start(send_two(i, b, turn))

    def reduced(i):
        settle(bulk_half, half_recv.at[i % ring, 0])
        for b in range(2):
            w = sizes[b][1]
            parts = held_here(b, i, 0, 0)
            parts = with_first(parts, i, b, 0)
            for turn in range(1, w):
                settle(bulk, two_recv.at[i, b, turn - 1])
                parts = [
                    p + decode(land_two[i, b, turn - 1, j], land_scale_two[i, b, turn - 1])
                    for j, p in enumerate(parts)
                ]
            pack(parts, out_three.at[i * 2 + b], out_scale_three.at[i * 2 + b])
        release(i)

    def third_hop(i):
        reduced(i)
        for b in range(2):
            start(send_three(i, b, chunk_group(i), group, core))

    spread(0)

    settle(land_far.at[pl.ds(0, groups - 1)], far_recv.at[0])

    total = groups * per_three
    pick = jnp.broadcast_to(group * per_three + lane % per_three, (ROWS, lanes))
    third = jnp.full((1, lanes), -1, jnp.int32)
    for u in range(groups):
        third = jnp.where(lane // per_three == u, lookup(land_far[u], pick)[4:5, :], third)
    down_third = column(third)

    def rank(k):
        return (group - k // per_three - 1 + groups) % groups * per_three + k % per_three

    rank_down, rank_across = rank(order_down), rank(order_across)
    real = order_down < total
    before = latest(real & (down_third == third) & (rank_down < rank_across), rank_down)
    last = latest(real & (down_third == order_across), rank_down)
    plan_third[0:1, :] = jnp.where(before < 0, total, before)
    plan_third[1:2, :] = jnp.where(last < 0, total, last)
    plan_third[2:, :] = jnp.zeros((plan_third.shape[0] - 2, lanes), jnp.int32)
    third_to_smem = pltpu.make_async_copy(plan_third, third_smem, local.at[0])
    third_to_smem.start()

    settle(land_weight.at[pl.ds(0, n - 1)], near_recv.at[1])

    held = weight[...]
    for step in range(1, n):
        held = held + land_weight[peer(step)]
    near_weight[...] = held

    @pl.loop(1, groups)
    def _(step):
        send_weight_far(far_peer(step), group).start()

    @pl.loop(0, groups)
    def _(i):
        first_hop(i)

        @pl.when(i > 0)
        def _():
            third_hop(i - 1)

        @pl.when(i + 1 < groups)
        def _():
            spread(i + 1)

        second_hop(i)

    owned = weight.shape[0]
    start_row = (group * n + me) * (owned // 4)
    for e in range(owned // 8):
        folded = jnp.zeros((ROWS, width), jnp.float32)
        for f in range(8 * e, 8 * e + 8):
            row = table[pl.ds(f % 4 * quarter + start_row + f // 4, 1), :]
            folded = folded + fold(weight[f : f + 1, :], row)
        coarse_weight[e : e + 1, :] = jnp.sum(folded, axis=0, keepdims=True)
    held = near_weight[...]
    settle(land_weight_far.at[pl.ds(0, groups - 1)], far_recv.at[1])
    for step in range(1, groups):
        held = held + land_weight_far[far_source(step)]
    whole = jnp.sum(jnp.sum(held, axis=0, keepdims=True), axis=1, keepdims=True)
    vertices = relative.shape[0] * n * groups * relative.shape[1]
    relative[...] = coarse_weight[...] * vertices / whole

    third_to_smem.wait()
    end = groups - 1

    def take(codes, scales, at, h, u):
        for j in range(per_three):
            part = decode(codes[j], scales[...])
            sums_three[at + j, h] = part + sums_three[third_smem[0, u * per_three + j], h]

    @pl.loop(1, groups)
    def _(step):
        u = far_source(step)
        for h in range(2):
            settle(bulk, three_recv.at[u, h])
            take(land_three.at[u, h], land_scale_three.at[u, h], (step - 1) * per_three, h, u)

    reduced(end)
    start(send_three(end, 1 - core, group, group, core))

    take(out_three.at[end * 2 + core], out_scale_three.at[end * 2 + core], end * per_three, core, group)
    other = 1 - core
    settle(bulk, three_recv.at[group, other])
    take(land_three.at[group, other], land_scale_three.at[group, other], end * per_three, other, group)

    @pl.loop(0, coarse.shape[0])
    def _(slot):
        coarse[slot] = sums_three[third_smem[1, slot]]

    settle(land_labels.at[pl.ds(0, n - 1)], near_send.at[0])
    settle(land_weight.at[pl.ds(0, n - 1)], near_send.at[1])
    settle(land_far.at[pl.ds(0, groups - 1)], far_send.at[0])
    settle(land_weight_far.at[pl.ds(0, groups - 1)], far_send.at[1])
    for at in range(ring):
        settle(out_half.at[at], half_send.at[at, 0])
        settle(out_scale_half.at[at], half_send.at[at, 1])
    for b in range(2):
        z, w = sizes[b]
        some, few = pl.ds(0, (z - 1) * w), pl.ds(0, w - 1)
        settle(out_one.at[pl.ds(0, groups), b, some], one_send.at[b, 0])
        settle(out_scale_one.at[pl.ds(0, groups), b, some], one_send.at[b, 1])
        settle(out_two.at[pl.ds(0, groups), b, few], two_send.at[b, 0])
        settle(out_scale_two.at[pl.ds(0, groups), b, few], two_send.at[b, 1])
    settle(out_three.at[pl.ds(0, 2 * groups - 1)], three_send.at[0])
    settle(out_scale_three.at[pl.ds(0, 2 * groups - 1)], three_send.at[1])


def hand_on(coarse_in, relative_in, coarse, relative, blocks, row, arrive, leave):
    pieces = arrive.shape[0] - 1
    size = blocks.shape[0] // pieces
    moves = [(coarse_in, blocks, coarse, pl.ds(i * size, size)) for i in range(pieces)]
    moves.append((relative_in, row, relative, pl.ds(0, row.shape[0])))
    ins = [pltpu.make_async_copy(a.at[p], v.at[p], arrive.at[i]) for i, (a, v, _, p) in enumerate(moves)]
    outs = [pltpu.make_async_copy(v.at[p], b.at[p], leave.at[i]) for i, (_, v, b, p) in enumerate(moves)]
    for copy in ins:
        copy.start()
    for first, second in zip(ins, outs):
        first.wait()
        second.start()
    for copy in outs:
        copy.wait()


VMEM = pl.BlockSpec(memory_space=pltpu.VMEM)
HBM = pl.BlockSpec(memory_space=pl.ANY)
VMEM_BYTES = 67_043_328


def per_device(
    blocks,
    ids_one,
    ids_two,
    ids_three,
    match_one,
    match_two,
    match_three,
    target_one,
    target_two,
    target_three,
    vertex_weights,
):
    n, groups = lax.axis_size("dev"), lax.axis_size("grp")
    count, width = blocks.shape[0], blocks.shape[1]
    rows = width // 2
    lanes = -(-count // width) * width
    owned = vertex_weights.shape[0]
    slots = count // 4
    per = slots // groups
    chips = n // 2
    across = 1
    while across * across < chips:
        across *= 2
    down = chips // across
    hop_one = max((across - 1) * down, (down - 1) * across, 1)
    hop_two = max(across - 1, down - 1, 1)
    plan_rows = -(-(1 + -(-n * slots // lanes)) // ROWS) * ROWS
    half_bytes = groups * chips * 4 * per * rows * width * 2
    ring = groups if half_bytes <= VMEM_BYTES // 4 else 2

    def message(*lead, per=per):
        return [
            pltpu.VMEM(lead + (per, rows, width), jnp.int16),
            pltpu.VMEM(lead + (1, width), jnp.float32),
        ] * 2

    targets = [x[None] for x in (target_one, target_two, target_three)]
    small = [ids_one, *targets, vertex_weights, match_one, match_two, match_three]
    coarse, relative = pl.pallas_call(
        functools.partial(coarsen, n, groups, across),
        in_specs=[HBM] * 9,
        out_specs=(VMEM, VMEM),
        out_shape=(
            jax.ShapeDtypeStruct((count // 8, 2, rows, width), jnp.float32),
            jax.ShapeDtypeStruct((owned // 8, width), jnp.float32),
        ),
        scratch_shapes=[
            pltpu.SMEM(ids_one.shape, jnp.int32),
            *[pltpu.VMEM(x.shape, x.dtype) for x in small],
            pltpu.VMEM(match_one.shape, jnp.int32),
            pltpu.VMEM((count, width, width), jnp.bfloat16),
            pltpu.VMEM((ROWS, lanes), jnp.int32),
            pltpu.VMEM((n, ROWS, lanes), jnp.int32),
            pltpu.VMEM((groups, ROWS, lanes), jnp.int32),
            pltpu.VMEM((n, owned, width), jnp.float32),
            pltpu.VMEM((owned, width), jnp.float32),
            pltpu.VMEM((groups, owned, width), jnp.float32),
            pltpu.VMEM((plan_rows, lanes), jnp.int32),
            pltpu.SMEM((plan_rows, lanes), jnp.int32),
            pltpu.VMEM((ROWS, lanes), jnp.int32),
            pltpu.SMEM((ROWS, lanes), jnp.int32),
            pltpu.VMEM((owned // 8, width), jnp.float32),
            pltpu.VMEM((count + 1, width, width), jnp.float32),
            *message(ring, chips, per=2 * per),
            *message(groups, 2, hop_one),
            *message(groups, 2, hop_two),
            *message(2 * groups)[:2],
            *message(groups, 2)[:2],
            pltpu.VMEM((groups * per + 1, 2, rows, width), jnp.float32),
            pltpu.VMEM((per * rows // 2 + 1, 1, width), jnp.float32),
            pltpu.VMEM((per * rows + 1, 1, width), jnp.float32),
            pltpu.SemaphoreType.DMA((2,)),
            pltpu.SemaphoreType.DMA((2,)),
            pltpu.SemaphoreType.DMA((2,)),
            pltpu.SemaphoreType.DMA((2,)),
            pltpu.SemaphoreType.DMA((ring, 2)),
            pltpu.SemaphoreType.DMA((ring, chips)),
            pltpu.SemaphoreType.DMA((2, 2)),
            pltpu.SemaphoreType.DMA((groups, 2, hop_one)),
            pltpu.SemaphoreType.DMA((2, 2)),
            pltpu.SemaphoreType.DMA((groups, 2, hop_two)),
            pltpu.SemaphoreType.DMA((2,)),
            pltpu.SemaphoreType.DMA((groups, 2)),
            pltpu.SemaphoreType.DMA((count // math.gcd(count, 16),)),
            pltpu.SemaphoreType.DMA((9,)),
            pltpu.SemaphoreType.DMA((2,)),
            pltpu.SemaphoreType.REGULAR,
        ],
        compiler_params=pltpu.CompilerParams(
            collective_id=0,
            has_side_effects=True,
            vmem_limit_bytes=VMEM_BYTES,
        ),
    )(
        blocks,
        *small,
    )
    pieces = math.gcd(count // 8, 4)
    coarse, relative = pl.pallas_call(
        hand_on,
        in_specs=[HBM, HBM],
        out_specs=(HBM, HBM),
        out_shape=(
            jax.ShapeDtypeStruct(coarse.shape, jnp.float32),
            jax.ShapeDtypeStruct(relative.shape, jnp.float32),
        ),
        scratch_shapes=[
            pltpu.VMEM(coarse.shape, jnp.float32),
            pltpu.VMEM(relative.shape, jnp.float32),
            pltpu.SemaphoreType.DMA((pieces + 1,)),
            pltpu.SemaphoreType.DMA((pieces + 1,)),
        ],
    )(coarse, relative)
    return coarse.reshape(count // 8, width, width), relative


def solution(mesh):
    both = ("grp", "dev")
    return jax.shard_map(
        per_device,
        mesh=mesh,
        in_specs=(
            P(both, None, None),
            P(None, both),
            P(None, both),
            P(None, both),
            P(),
            P(),
            P(),
            P(both),
            P(both),
            P(both),
            P(both, None),
        ),
        out_specs=(P(both, None, None), P(both, None)),
        check_vma=False,
    )
```
